32 devices in a mesh: band: 4 (over y, x), ga: 8 (over z, core).
Axes of the slice: x: 2, y: 2, z: 4, core: 2. Of those that a mesh axis runs over, the one named last changes fastest.
Arguments:
- wavefunctions: bfloat16 [512, 98304], P('band', 'ga'), may hold values from -6 to 6
- projectors: bfloat16 [2048, 98304], P('band', 'ga'), may hold values from -0.125 to 0.125
- kinetic_diag: float32 [98304], P('ga'), may hold values from 0.1 to 4
- species_index: int32 [256], replicated, may hold values from 0 to 3
- coupling: float32 [4, 8, 8], replicated, may hold values from -5 to 5
Outputs:
- applied: bfloat16 [512, 98304], P('band', 'ga')
The draws below stay inside these ranges and needn't reach their ends.
All inputs are finite; a program needn't handle non-finite values.
Results may differ from the reference program's by a relative error of at most 0.015.
Values may be sent and summed in bfloat16 or wider, within the bound.
A program may use at most 64 MiB of HBM per device.

```python
import math
import jax
import jax.numpy as jnp
from jax import lax

NG = 98304
NPA = 8
ATOMS = 256
NSPEC = 4
BANDS = 512
NPROJ = 2048


def place_ends(array, rng, low, top_value):
    longest = array.shape.index(max(array.shape))
    spots = []
    for shift in (0, 1):
        where = [jax.random.randint(jax.random.fold_in(rng, axis), (), 0, length) for axis, length in enumerate(array.shape)]
        where[longest] = (where[longest] + shift) % array.shape[longest]
        spots.append(tuple(where))
    return array.at[spots[0]].set(low).at[spots[1]].set(top_value)


def shard_levels(rng, extent, split, smallest, largest):
    def one(axis_at, shards_of):
        steps = jax.random.uniform(jax.random.fold_in(jax.random.fold_in(rng, 6), axis_at), (shards_of,), jnp.float32, smallest / len(split), largest / len(split))
        return jnp.repeat(jnp.exp(steps), extent[axis_at] // shards_of).reshape((-1,) + (1,) * (len(extent) - axis_at - 1))

    gain = one(*split[0])
    for cut in split[1:]:
        gain = gain * one(*cut)
    return gain


def noise(rng, dims, spread, reach, shards=(), held_as=jnp.bfloat16):
    values = spread * jax.random.normal(rng, dims, jnp.float32)
    if shards:
        values = values * shard_levels(rng, dims, shards, -0.22, 0.18)
    return jnp.clip(values, -reach, reach).astype(held_as)


def setup_inputs(seed: int = 0) -> dict:
    splits = jax.random.split(jax.random.key(seed), 6)
    return {
        "wavefunctions": noise(splits[0], (BANDS, NG), 1.0, 6.0, ((0, 4), (1, 8))),
        "projectors": noise(splits[1], (NPROJ, NG), ((NG * NPROJ) ** -0.25), 0.125, ((0, 4), (1, 8))),
        "kinetic_diag": jnp.clip(jnp.exp(math.log(4.0) - 3.6888794 * jax.random.uniform(splits[2], (NG,), jnp.float32) ** shard_levels(splits[2], (NG,), ((0, 8),), -0.2, 0.2)), 0.1, 4.0),
        "species_index": place_ends(jax.random.randint(splits[3], (ATOMS,), 0, NSPEC), jax.random.fold_in(splits[3], 1), 0, NSPEC - 1).astype(jnp.int32),
        "coupling": noise(splits[4], (NSPEC, NPA, NPA), 0.35, 5.0, (), jnp.float32),
    }


def reference(wavefunctions, projectors, kinetic_diag, species_index, coupling):
    correlations = jnp.dot(wavefunctions, projectors.T, preferred_element_type=jnp.float32)
    onehot = (species_index[:, None] == jnp.arange(NSPEC, dtype=jnp.int32)[None, :]).astype(jnp.float32)
    blocks = jnp.einsum("as,sij->aij", onehot, coupling, precision=lax.Precision.HIGHEST)
    mixed = jnp.einsum("baj,aij->bai", correlations.reshape(BANDS, ATOMS, NPA), blocks, precision=lax.Precision.HIGHEST)
    mixed = mixed.reshape(BANDS, NPROJ).astype(jnp.bfloat16)
    nonlocal_term = jnp.dot(mixed, projectors, preferred_element_type=jnp.float32)
    return (kinetic_diag[None, :] * wavefunctions.astype(jnp.float32) + nonlocal_term).astype(jnp.bfloat16)
```

```python
import functools

import jax
import jax.numpy as jnp
from jax import lax
from jax.experimental import pallas as pl
from jax.experimental.pallas import tpu as pltpu
from jax.sharding import PartitionSpec as P

CHUNKS = 4
TILES = 4
PIECES = 8
LANES = 128

NPA = 8


def apply_blocks(correlations, species_index, coupling, atom_start):
    rows = correlations.shape[0]
    count = correlations.shape[1] // NPA
    local_species = lax.dynamic_slice_in_dim(species_index, atom_start, count)
    onehot = (
        local_species[:, None] == jnp.arange(coupling.shape[0], dtype=jnp.int32)[None, :]
    ).astype(jnp.float32)
    blocks = jnp.einsum("as,sij->aij", onehot, coupling, precision=lax.Precision.HIGHEST)
    mixed = jnp.einsum(
        "baj,aij->bai",
        correlations.reshape(rows, count, NPA),
        blocks,
        precision=lax.Precision.HIGHEST,
    )
    return mixed.reshape(rows, count * NPA).astype(jnp.bfloat16)


def reduce_and_mix(partial_value, species_index, coupling, first_proj):
    total = lax.psum(partial_value.astype(jnp.bfloat16), "ga").astype(jnp.float32)
    return apply_blocks(total, species_index, coupling, first_proj // NPA)


def local(wavefunctions, projectors, kinetic_diag, species_index, coupling):
    proj_local = projectors.shape[0]
    band_index = lax.axis_index("band")
    partial_value = jnp.einsum(
        "bg,pg->bp",
        lax.all_gather(wavefunctions, "band", axis=0, tiled=True),
        projectors,
        preferred_element_type=jnp.float32,
    )
    mixed = reduce_and_mix(partial_value, species_index, coupling, band_index * proj_local)
    nonlocal_term = lax.psum_scatter(
        jnp.dot(mixed, projectors, preferred_element_type=jnp.float32).astype(jnp.bfloat16),
        "band",
        scatter_dimension=0,
        tiled=True,
    ).astype(jnp.float32)
    return (kinetic_diag[None, :] * wavefunctions.astype(jnp.float32) + nonlocal_term).astype(
        jnp.bfloat16
    )


def schedule(chunks):
    period = 50.0 / chunks
    events = []
    for k in range(chunks):
        ready = 0.0 if k == 0 else k * period + 4.0
        if k > 0:
            events.append((ready - 10.0, "forward", k))
        events.append((ready, "correlate", k))
        events.append((ready + 10.0, "reduce", k))
        events.append((ready + 12.5, "join", k))
        events.append((ready + 13.7, "mix", k))
        if k == 0:
            events.append((ready + 13.8, "feed", k))
        events.append((ready + 16.0, "share", k))
        events.append((ready + 26.0, "expand", k))
        for t in range(TILES):
            events.append((ready + 38.0 + 2.5 * t, "finish", (k, t)))
    return [event[1:] for event in sorted(events, key=lambda event: event[0])]


def kernel(
    nga, wf, pj, kin_hbm, species_hbm, coupling_hbm, out,
    proj, wave, acc, csend, keep, parts, msend, mrecv, dsend, drecv, mixed,
    nsend, nrecv, own, nfull, kin, species, coupling, tiles,
    s_loc, s_p, s_wm, s_wo, s_wf, s_z, s_m, s_d, s_b, s_e, s_g, s_n, s_o,
):
    chunks, _, rows, half = wave.shape
    _, zn, share, both = csend.shape
    count = both // 2
    width = nsend.shape[-1]
    piece = half // PIECES
    quarter = zn // 4
    band, me = lax.axis_index("band"), lax.axis_index("ga")
    core, z, y, x = me % 2, me // 2, band // 2, band % 2
    across_x, across_y, diag = y * 2 + 1 - x, (1 - y) * 2 + x, 3 - band
    m = (1 - core) * y + core * x
    m_nbr = (1 - core) * across_y + core * across_x
    o_nbr = (1 - core) * across_x + core * across_y
    here = pl.multiple_of(m * half, LANES)
    there = pl.multiple_of((1 - m) * half, LANES)
    to_m, to_o, to_twin = {"band": m_nbr}, {"band": o_nbr}, {"ga": z * 2 + 1 - core}

    def remote(src, dst, sems, device):
        return pltpu.make_async_remote_copy(
            src_ref=src, dst_ref=dst, send_sem=sems.at[0], recv_sem=sems.at[1],
            device_id=device, device_id_type=pl.DeviceIdType.MESH,
        )

    def span(k):
        return pl.ds(k * rows, rows)

    def peer(step):
        return (z + 1 + step) % zn

    def to_peer(step):
        return {"ga": peer(step) * 2 + core}

    local_p = pltpu.make_async_copy(pj.at[:, pl.ds(here, half)], proj.at[0], s_loc.at[0])
    local_k = pltpu.make_async_copy(kin_hbm.at[:, pl.ds(here, half)], kin, s_loc.at[1])
    local_s = pltpu.make_async_copy(species_hbm, species, s_loc.at[2])
    local_c = pltpu.make_async_copy(coupling_hbm, coupling, s_loc.at[3])
    local_w = [
        pltpu.make_async_copy(wf.at[span(k), pl.ds(here, half)], wave.at[k, band], s_loc.at[4 + k])
        for k in range(chunks)
    ]
    send_p = [
        remote(
            pj.at[:, pl.ds(pl.multiple_of(there + i * piece, LANES), piece)],
            proj.at[1, :, pl.ds(i * piece, piece)], s_p.at[i], to_m,
        )
        for i in range(PIECES)
    ]
    send_wm = [
        remote(wf.at[span(k), pl.ds(there, half)], wave.at[k, band], s_wm.at[k], to_m)
        for k in range(chunks)
    ]
    send_wo = [
        remote(wf.at[span(k), pl.ds(here, half)], wave.at[k, band], s_wo.at[k], to_o)
        for k in range(chunks)
    ]
    send_wf = [
        remote(wave.at[k, m_nbr], wave.at[k, m_nbr], s_wf.at[k], to_o) for k in range(chunks)
    ]
    send_m = [remote(msend.at[k], mrecv.at[k], s_m.at[k], to_m) for k in range(chunks)]
    send_d = [remote(dsend.at[k], drecv.at[k], s_d.at[k], to_twin) for k in range(chunks)]
    send_b = [
        remote(mixed.at[k, z, :, :count], mixed.at[k, z, :, count:], s_b.at[k], to_m)
        for k in range(chunks)
    ]

    def send_z(k, step):
        return remote(
            csend.at[k, peer(step)], parts.at[k, step], s_z.at[k, step], to_peer(step)
        )

    def send_e(k, step):
        place = mixed.at[k, z, :, :count]
        return remote(place, place, s_e.at[k, step], to_peer(step))

    def send_g(k, step):
        place = mixed.at[k, z, :, count:]
        return remote(place, place, s_g.at[k, step], to_peer(step))

    def send_n(k, t):
        return remote(nsend.at[k, t], nrecv.at[k, t], s_n.at[k, t], to_o)

    def send_o(k, t):
        place = out.at[span(k), pl.ds(pl.multiple_of(here + t * width, LANES), width)]
        return remote(nfull.at[k, t], place, s_o.at[k, t], to_m)

    def each_peer(body):
        def step(i, carry):
            body(i)
            return carry

        lax.fori_loop(0, zn - 1, step, 0)

    def each_tile(body):
        def step(i, carry):
            body(i)
            return carry

        lax.fori_loop(0, TILES, step, 0)

    def columns(t):
        return pl.ds(pl.multiple_of(t * width, LANES), width)

    def add_product(k, slot, cols):
        product = lax.dot_general(
            wave[k, :, :, cols].reshape(4 * rows, -1),
            proj[slot, :, cols],
            (((1,), (1,)), ((), ())),
            preferred_element_type=jnp.float32,
        )
        acc[:, :, slot * count : (slot + 1) * count] += product.reshape(zn, share, count)

    def build_tiles():
        kinds, npa = coupling.shape[0], coupling.shape[1]
        atoms = species.shape[1]
        local_s.wait()
        local_c.wait()
        first = band * (count // npa)
        atom = lax.broadcasted_iota(jnp.int32, (atoms, count), 0)
        column = lax.broadcasted_iota(jnp.int32, (atoms, count), 1)
        spread = (atom == first + column // npa).astype(jnp.float32)
        kind = lax.broadcasted_iota(jnp.int32, (8, atoms), 0)
        onehot = (kind == species[...]).astype(jnp.float32)
        chosen = jnp.dot(
            onehot, spread, preferred_element_type=jnp.float32, precision=lax.Precision.HIGHEST
        )
        row = lax.broadcasted_iota(jnp.int32, (LANES, npa), 0)
        index = lax.broadcasted_iota(jnp.int32, (LANES, npa), 1)
        repeat = (row % npa == index).astype(jnp.float32)
        blocks = []
        for s in range(kinds):
            tall = lax.dot_general(
                repeat, coupling[s], (((1,), (1,)), ((), ())),
                preferred_element_type=jnp.float32, precision=lax.Precision.HIGHEST,
            )
            blocks.append(
                lax.dot_general(
                    tall, repeat, (((1,), (1,)), ((), ())),
                    preferred_element_type=jnp.float32, precision=lax.Precision.HIGHEST,
                )
            )
        atom_row = lax.broadcasted_iota(jnp.int32, (LANES, LANES), 0) // npa
        atom_col = lax.broadcasted_iota(jnp.int32, (LANES, LANES), 1) // npa
        same = atom_row == atom_col
        for t in range(tiles.shape[0]):
            value = jnp.zeros((LANES, LANES), jnp.float32)
            for s in range(kinds):
                here_kind = chosen[s : s + 1, t * LANES : (t + 1) * LANES]
                value = jnp.where(here_kind > 0.5, blocks[s], value)
            tiles[t] = jnp.where(same, value, 0.0)

    def forward(k):
        send_wm[k].wait_recv()
        send_wf[k].start()

    def feed(k):
        for later in range(2, chunks):
            send_wm[later].start()

    def correlate(k):
        if k > 0:
            local_w[k].wait()
            send_wo[k].wait_recv()
            send_wf[k].wait_recv()
            acc[...] = jnp.zeros_like(acc)

            def tile(t):
                add_product(k, 0, columns(t))
                add_product(k, 1, columns(t))

            each_tile(tile)
        csend[k] = acc[...].astype(jnp.bfloat16)
        each_peer(lambda step: send_z(k, step).start())
        keep[k] = acc[z]

    def reduce(k):
        each_peer(lambda step: send_z(k, step).wait_recv())
        total = keep[k]
        for step in range(zn - 1):
            total = total + parts[k, step].astype(jnp.float32)
        msend[k] = total[:, count:].astype(jnp.bfloat16)
        send_m[k].start()
        dsend[k] = total[:, :count]

    def join(k):
        send_m[k].wait_recv()
        dsend[k] = dsend[k] + mrecv[k].astype(jnp.float32)
        send_d[k].start()

    def mix(k):
        send_d[k].wait_recv()
        total = dsend[k] + drecv[k]
        for t in range(tiles.shape[0]):
            cols = slice(t * LANES, (t + 1) * LANES)
            mixed[k, z, :, cols] = jnp.dot(
                total[:, cols], tiles[t],
                preferred_element_type=jnp.float32, precision=lax.Precision.HIGHEST,
            ).astype(jnp.bfloat16)
        send_b[k].start()
        each_peer(lambda step: send_e(k, step).start())

    def share_out(k):
        send_b[k].wait_recv()
        each_peer(lambda step: send_g(k, step).start())

    def expand(k):
        each_peer(lambda step: send_e(k, step).wait_recv())
        each_peer(lambda step: send_g(k, step).wait_recv())

        def tile(t):
            cols = columns(t)
            picks = [
                mixed[k, pl.ds(b * quarter, quarter)].reshape(rows, both)
                for b in (o_nbr, diag, band, m_nbr)
            ]
            value = jnp.dot(
                jnp.concatenate(picks, axis=0), proj[:, :, cols].reshape(both, width),
                preferred_element_type=jnp.float32,
            ).reshape(4, rows, width)
            nsend[k, t] = value[:2].astype(jnp.bfloat16)
            send_n(k, t).start()
            own[k, t] = value[2:]

        each_tile(tile)

    def finish(k, t):
        send_n(k, t).wait_recv()
        cols = columns(t)
        scale = kin[:, cols]
        value = own[k, t] + nrecv[k, t].astype(jnp.float32)
        theirs = scale * wave[k, m_nbr, :, cols].astype(jnp.float32) + value[1]
        nfull[k, t] = theirs.astype(jnp.bfloat16)
        send_o(k, t).start()
        mine = scale * wave[k, band, :, cols].astype(jnp.float32) + value[0]
        place = pl.ds(pl.multiple_of(here + t * width, LANES), width)
        out[span(k), place] = mine.astype(jnp.bfloat16)

    barrier = pltpu.get_barrier_semaphore()
    for device in (to_m, to_o, to_twin):
        pl.semaphore_signal(
            barrier, inc=1, device_id=device, device_id_type=pl.DeviceIdType.MESH
        )
    each_peer(
        lambda step: pl.semaphore_signal(
            barrier, inc=1, device_id=to_peer(step), device_id_type=pl.DeviceIdType.MESH
        )
    )
    local_p.start()
    for copy in local_w:
        copy.start()
    local_s.start()
    local_c.start()
    local_k.start()
    pl.semaphore_wait(barrier, zn + 2)

    send_wm[0].start()
    send_wo[0].start()
    for copy in send_p:
        copy.start()
    send_wm[1].start()
    build_tiles()
    forward(0)
    local_k.wait()
    local_p.wait()
    local_w[0].wait()
    send_wo[0].wait_recv()
    send_wf[0].wait_recv()
    acc[...] = jnp.zeros_like(acc)
    each_tile(lambda t: add_product(0, 0, columns(t)))
    for i in range(PIECES):
        send_p[i].wait_recv()
        if i == PIECES - 2:
            for k in range(1, chunks):
                send_wo[k].start()
        add_product(0, 1, slice(i * piece, (i + 1) * piece))

    stages = {
        "forward": forward, "correlate": correlate, "reduce": reduce, "join": join,
        "mix": mix, "feed": feed, "share": share_out, "expand": expand,
    }
    for stage, at in schedule(chunks):
        if stage == "finish":
            finish(*at)
        else:
            stages[stage](at)

    for copy in send_p:
        copy.wait_send()
    for k in range(chunks):
        for copy in (send_wm[k], send_wo[k], send_wf[k], send_m[k], send_d[k], send_b[k]):
            copy.wait_send()
        for send in (send_z, send_e, send_g):
            each_peer(lambda step: send(k, step).wait_send())
        each_tile(lambda t: send_n(k, t).wait_send())
        each_tile(lambda t: send_o(k, t).wait())


def square(nga, wavefunctions, projectors, kinetic_diag, species_index, coupling):
    bands, waves = wavefunctions.shape
    count = projectors.shape[0]
    atoms = species_index.shape[0]
    half, rows = waves // 2, bands // CHUNKS
    zn = nga // 2
    width, share = half // TILES, 4 * rows // zn
    bf16, f32 = jnp.bfloat16, jnp.float32
    dma = pltpu.SemaphoreType.DMA
    anywhere = pl.BlockSpec(memory_space=pl.ANY)
    return pl.pallas_call(
        functools.partial(kernel, nga),
        out_shape=jax.ShapeDtypeStruct((bands, waves), bf16),
        in_specs=[anywhere] * 5,
        out_specs=pl.BlockSpec(memory_space=pltpu.VMEM),
        scratch_shapes=[
            pltpu.VMEM((2, count, half), bf16),
            pltpu.VMEM((CHUNKS, 4, rows, half), bf16),
            pltpu.VMEM((zn, share, 2 * count), f32),
            pltpu.VMEM((CHUNKS, zn, share, 2 * count), bf16),
            pltpu.VMEM((CHUNKS, share, 2 * count), f32),
            pltpu.VMEM((CHUNKS, zn - 1, share, 2 * count), bf16),
            pltpu.VMEM((CHUNKS, share, count), bf16),
            pltpu.VMEM((CHUNKS, share, count), bf16),
            pltpu.VMEM((CHUNKS, share, count), f32),
            pltpu.VMEM((CHUNKS, share, count), f32),
            pltpu.VMEM((CHUNKS, zn, share, 2 * count), bf16),
            pltpu.VMEM((CHUNKS, TILES, 2, rows, width), bf16),
            pltpu.VMEM((CHUNKS, TILES, 2, rows, width), bf16),
            pltpu.VMEM((CHUNKS, TILES, 2, rows, width), f32),
            pltpu.VMEM((CHUNKS, TILES, rows, width), bf16),
            pltpu.VMEM((1, half), f32),
            pltpu.VMEM((1, atoms), jnp.int32),
            pltpu.VMEM(coupling.shape, f32),
            pltpu.VMEM((count // LANES, LANES, LANES), f32),
            dma((4 + CHUNKS,)),
            dma((PIECES, 2)),
            dma((CHUNKS, 2)),
            dma((CHUNKS, 2)),
            dma((CHUNKS, 2)),
            dma((CHUNKS, zn - 1, 2)),
            dma((CHUNKS, 2)),
            dma((CHUNKS, 2)),
            dma((CHUNKS, 2)),
            dma((CHUNKS, zn - 1, 2)),
            dma((CHUNKS, zn - 1, 2)),
            dma((CHUNKS, TILES, 2)),
            dma((CHUNKS, TILES, 2)),
        ],
        compiler_params=pltpu.CompilerParams(
            collective_id=0, has_side_effects=True, vmem_limit_bytes=50 * 2**20
        ),
    )(
        wavefunctions, projectors, kinetic_diag.reshape(1, waves),
        species_index.reshape(1, atoms), coupling,
    )


def solution(mesh):
    in_specs = (P("band", "ga"), P("band", "ga"), P("ga"), P(), P())
    out_specs = P("band", "ga")
    nga = mesh.shape["ga"]
    fits = mesh.shape["band"] == 4 and nga % 8 == 0
    body = functools.partial(square, nga) if fits else local
    return jax.shard_map(body, mesh=mesh, in_specs=in_specs, out_specs=out_specs, check_vma=False)
```

```python
import functools

import jax
import jax.numpy as jnp
from jax import lax
from jax.experimental import pallas as pl
from jax.experimental.pallas import tpu as pltpu
from jax.sharding import PartitionSpec as P

CHUNKS = 4
TILES = 4
PIECES = 8
LANES = 128

NPA = 8


def apply_blocks(correlations, species_index, coupling, atom_start):
    rows = correlations.shape[0]
    count = correlations.shape[1] // NPA
    local_species = lax.dynamic_slice_in_dim(species_index, atom_start, count)
    onehot = (
        local_species[:, None] == jnp.arange(coupling.shape[0], dtype=jnp.int32)[None, :]
    ).astype(jnp.float32)
    blocks = jnp.einsum("as,sij->aij", onehot, coupling, precision=lax.Precision.HIGHEST)
    mixed = jnp.einsum(
        "baj,aij->bai",
        correlations.reshape(rows, count, NPA),
        blocks,
        precision=lax.Precision.HIGHEST,
    )
    return mixed.reshape(rows, count * NPA).astype(jnp.bfloat16)


def reduce_and_mix(partial_value, species_index, coupling, first_proj):
    total = lax.psum(partial_value.astype(jnp.bfloat16), "ga").astype(jnp.float32)
    return apply_blocks(total, species_index, coupling, first_proj // NPA)


def local(wavefunctions, projectors, kinetic_diag, species_index, coupling):
    proj_local = projectors.shape[0]
    band_index = lax.axis_index("band")
    partial_value = jnp.einsum(
        "bg,pg->bp",
        lax.all_gather(wavefunctions, "band", axis=0, tiled=True),
        projectors,
        preferred_element_type=jnp.float32,
    )
    mixed = reduce_and_mix(partial_value, species_index, coupling, band_index * proj_local)
    nonlocal_term = lax.psum_scatter(
        jnp.dot(mixed, projectors, preferred_element_type=jnp.float32).astype(jnp.bfloat16),
        "band",
        scatter_dimension=0,
        tiled=True,
    ).astype(jnp.float32)
    return (kinetic_diag[None, :] * wavefunctions.astype(jnp.float32) + nonlocal_term).astype(
        jnp.bfloat16
    )


EARLY = 2


def schedule():
    times = {
        "correlate": (0.3, 0.5, 16.5, 24.6),
        "forward": (None, None, 4.0, 9.5),
        "reduce": (7.5, 12.0, 29.3, 37.4),
        "join": (9.7, 15.0, 32.2, 40.0),
        "mix": (11.3, 21.2, 33.4, 41.2),
        "share": (14.4, 24.0, 36.0, 44.0),
        "expand": (21.5, 29.6, 42.0, 50.0),
        "settle": (57.0, None, None, None),
    }
    events = [
        (at, stage, k, 0)
        for stage, row in times.items()
        for k, at in enumerate(row)
        if at is not None
    ]
    for k, (first, step) in enumerate(((29.5, 0.02), (36.5, 1.2), (50.5, 1.2), (62.0, 1.0))):
        events += [(first + step * t, "far", k, t) for t in range(TILES)]
    for k, first in enumerate((44.2, 52.6, 58.0, 70.0)):
        events += [(first + 0.05 * t, "near", k, t) for t in range(TILES)]
    return [event[1:] for event in sorted(events)]


def kernel(
    nga, wf, pj, kin_hbm, species_hbm, coupling_hbm, out,
    proj, wave, acc, csend, keep, parts, msend, mrecv, dsend, drecv, mixed,
    nsend, nrecv, own, nfull, ready, kin, species, coupling, tiles,
    s_loc, s_p, s_wm, s_wo, s_wf, s_z, s_m, s_d, s_b, s_e, s_g, s_n, s_o, s_w,
):
    chunks, _, rows, half = wave.shape
    _, zn, share, both = csend.shape
    count = both // 2
    width = nsend.shape[-1]
    piece = half // PIECES
    quarter = zn // 4
    band, me = lax.axis_index("band"), lax.axis_index("ga")
    core, z, y, x = me % 2, me // 2, band // 2, band % 2
    across_x, across_y, diag = y * 2 + 1 - x, (1 - y) * 2 + x, 3 - band
    m = (1 - core) * y + core * x
    m_nbr = (1 - core) * across_y + core * across_x
    o_nbr = (1 - core) * across_x + core * across_y
    here = pl.multiple_of(m * half, LANES)
    there = pl.multiple_of((1 - m) * half, LANES)
    to_m, to_o, to_twin = {"band": m_nbr}, {"band": o_nbr}, {"ga": z * 2 + 1 - core}

    def remote(src, dst, sems, device):
        return pltpu.make_async_remote_copy(
            src_ref=src, dst_ref=dst, send_sem=sems.at[0], recv_sem=sems.at[1],
            device_id=device, device_id_type=pl.DeviceIdType.MESH,
        )

    def span(k):
        return pl.ds(k * rows, rows)

    def peer(step):
        return (z + 1 + step) % zn

    def to_peer(step):
        return {"ga": peer(step) * 2 + core}

    local_p = pltpu.make_async_copy(pj.at[:, pl.ds(here, half)], proj.at[0], s_loc.at[0])
    local_k = pltpu.make_async_copy(kin_hbm.at[:, pl.ds(here, half)], kin, s_loc.at[1])
    local_s = pltpu.make_async_copy(species_hbm, species, s_loc.at[2])
    local_c = pltpu.make_async_copy(coupling_hbm, coupling, s_loc.at[3])
    local_w = [
        pltpu.make_async_copy(wf.at[span(k), pl.ds(here, half)], wave.at[k, band], s_loc.at[4 + k])
        for k in range(chunks)
    ]
    send_p = [
        remote(
            pj.at[:, pl.ds(pl.multiple_of(there + i * piece, LANES), piece)],
            proj.at[1, :, pl.ds(i * piece, piece)], s_p.at[i], to_m,
        )
        for i in range(PIECES)
    ]
    send_wm = [
        remote(wf.at[span(k), pl.ds(there, half)], wave.at[k, band], s_wm.at[k], to_m)
        for k in range(chunks)
    ]
    send_wo = [
        remote(wf.at[span(k), pl.ds(here, half)], wave.at[k, band], s_wo.at[k], to_o)
        for k in range(chunks)
    ]
    send_wf = [
        remote(wave.at[k, m_nbr], wave.at[k, m_nbr], s_wf.at[k], to_o) for k in range(chunks)
    ]
    send_m = [remote(msend.at[k], mrecv.at[k], s_m.at[k], to_m) for k in range(chunks)]
    send_d = [remote(dsend.at[k], drecv.at[k], s_d.at[k], to_twin) for k in range(chunks)]
    send_b = [
        remote(mixed.at[k, z, :, :count], mixed.at[k, z, :, count:], s_b.at[k], to_m)
        for k in range(chunks)
    ]

    def send_z(k, step):
        return remote(
            csend.at[k, peer(step)], parts.at[k, step], s_z.at[k, step], to_peer(step)
        )

    def send_e(k, step):
        place = mixed.at[k, z, :, :count]
        return remote(place, place, s_e.at[k, step], to_peer(step))

    def send_g(k, step):
        place = mixed.at[k, z, :, count:]
        return remote(place, place, s_g.at[k, step], to_peer(step))

    def send_n(k, t, side):
        return remote(nsend.at[k, t, side], nrecv.at[k, t, side], s_n.at[k, t, side], to_o)

    def place(k, t):
        return out.at[span(k), pl.ds(pl.multiple_of(here + t * width, LANES), width)]

    def send_o(k, t):
        return remote(nfull.at[k, t], place(k, t), s_o.at[k, t], to_m)

    def write(k, t):
        return pltpu.make_async_copy(ready.at[k, t], place(k, t), s_w.at[k, t])

    def each_peer(body):
        def step(i, carry):
            body(i)
            return carry

        lax.fori_loop(0, zn - 1, step, 0)

    def each_tile(body):
        def step(i, carry):
            body(i)
            return carry

        lax.fori_loop(0, TILES, step, 0)

    def columns(t):
        return pl.ds(pl.multiple_of(t * width, LANES), width)

    def add_product(chunk, slot, cols):
        product = lax.dot_general(
            wave[chunk, :, :, cols].reshape(-1, proj[slot, :, cols].shape[-1]),
            proj[slot, :, cols],
            (((1,), (1,)), ((), ())),
            preferred_element_type=jnp.float32,
        )
        product = product.reshape(-1, zn, share, count)
        acc[: product.shape[0], :, :, slot * count : (slot + 1) * count] += product

    def build_tiles():
        kinds, npa = coupling.shape[0], coupling.shape[1]
        atoms = species.shape[1]
        local_s.wait()
        local_c.wait()
        first = band * (count // npa)
        atom = lax.broadcasted_iota(jnp.int32, (atoms, count), 0)
        column = lax.broadcasted_iota(jnp.int32, (atoms, count), 1)
        spread = (atom == first + column // npa).astype(jnp.float32)
        kind = lax.broadcasted_iota(jnp.int32, (8, atoms), 0)
        onehot = (kind == species[...]).astype(jnp.float32)
        chosen = jnp.dot(
            onehot, spread, preferred_element_type=jnp.float32, precision=lax.Precision.HIGHEST
        )
        row = lax.broadcasted_iota(jnp.int32, (LANES, npa), 0)
        index = lax.broadcasted_iota(jnp.int32, (LANES, npa), 1)
        repeat = (row % npa == index).astype(jnp.float32)
        blocks = []
        for s in range(kinds):
            tall = lax.dot_general(
                repeat, coupling[s], (((1,), (1,)), ((), ())),
                preferred_element_type=jnp.float32, precision=lax.Precision.HIGHEST,
            )
            blocks.append(
                lax.dot_general(
                    tall, repeat, (((1,), (1,)), ((), ())),
                    preferred_element_type=jnp.float32, precision=lax.Precision.HIGHEST,
                )
            )
        atom_row = lax.broadcasted_iota(jnp.int32, (LANES, LANES), 0) // npa
        atom_col = lax.broadcasted_iota(jnp.int32, (LANES, LANES), 1) // npa
        same = atom_row == atom_col
        for t in range(tiles.shape[0]):
            value = jnp.zeros((LANES, LANES), jnp.float32)
            for s in range(kinds):
                here_kind = chosen[s : s + 1, t * LANES : (t + 1) * LANES]
                value = jnp.where(here_kind > 0.5, blocks[s], value)
            tiles[t] = jnp.where(same, value, 0.0)

    def forward(k):
        send_wm[k].wait_recv()
        if k == EARLY:
            send_wo[k].start()
        send_wf[k].start()
        if k == EARLY:
            for later in range(EARLY + 1, chunks):
                send_wo[later].start()

    def correlate(k):
        place = k
        if k >= EARLY:
            place = 0
            local_w[k].wait()
            send_wo[k].wait_recv()
            send_wf[k].wait_recv()
            acc[0] = jnp.zeros_like(acc[0])

            def tile(t):
                add_product(slice(k, k + 1), 0, columns(t))
                add_product(slice(k, k + 1), 1, columns(t))

            each_tile(tile)
        csend[k] = acc[place].astype(jnp.bfloat16)
        each_peer(lambda step: send_z(k, step).start())
        keep[k] = acc[place, z]

    def reduce(k):
        each_peer(lambda step: send_z(k, step).wait_recv())
        total = keep[k]
        for step in range(zn - 1):
            total = total + parts[k, step].astype(jnp.float32)
        msend[k] = total[:, count:].astype(jnp.bfloat16)
        send_m[k].start()
        dsend[k] = total[:, :count]

    def join(k):
        send_m[k].wait_recv()
        dsend[k] = dsend[k] + mrecv[k].astype(jnp.float32)
        send_d[k].start()

    def mix(k):
        send_d[k].wait_recv()
        total = dsend[k] + drecv[k]
        for t in range(tiles.shape[0]):
            cols = slice(t * LANES, (t + 1) * LANES)
            mixed[k, z, :, cols] = jnp.dot(
                total[:, cols], tiles[t],
                preferred_element_type=jnp.float32, precision=lax.Precision.HIGHEST,
            ).astype(jnp.bfloat16)
        send_b[k].start()
        each_peer(lambda step: send_e(k, step).start())

    def share_out(k):
        send_b[k].wait_recv()
        each_peer(lambda step: send_g(k, step).start())

    def expand(k):
        each_peer(lambda step: send_e(k, step).wait_recv())
        each_peer(lambda step: send_g(k, step).wait_recv())

        def tile(t):
            cols = columns(t)
            picks = [
                mixed[k, pl.ds(b * quarter, quarter)].reshape(rows, both)
                for b in (o_nbr, diag, band, m_nbr)
            ]
            value = jnp.dot(
                jnp.concatenate(picks, axis=0), proj[:, :, cols].reshape(both, width),
                preferred_element_type=jnp.float32,
            ).reshape(4, rows, width)
            nsend[k, t] = value[:2].astype(jnp.bfloat16)
            send_n(k, t, 1).start()
            own[k, t] = value[2:]

        each_tile(tile)
        each_tile(lambda t: send_n(k, t, 0).start())

    def complete(k, t, side, owner):
        send_n(k, t, side).wait_recv()
        cols = columns(t)
        kinetic = kin[:, cols] * wave[k, owner, :, cols].astype(jnp.float32)
        total = own[k, t, side] + nrecv[k, t, side].astype(jnp.float32)
        return (kinetic + total).astype(jnp.bfloat16)

    def far(k, t):
        nfull[k, t] = complete(k, t, 1, m_nbr)
        send_o(k, t).start()

    def near(k, t):
        ready[k, t] = complete(k, t, 0, band)
        write(k, t).start()

    barrier = pltpu.get_barrier_semaphore()
    for device in (to_m, to_o, to_twin):
        pl.semaphore_signal(
            barrier, inc=1, device_id=device, device_id_type=pl.DeviceIdType.MESH
        )
    each_peer(
        lambda step: pl.semaphore_signal(
            barrier, inc=1, device_id=to_peer(step), device_id_type=pl.DeviceIdType.MESH
        )
    )
    local_p.start()
    for copy in local_w:
        copy.start()
    local_s.start()
    local_c.start()
    local_k.start()
    pl.semaphore_wait(barrier, zn + 2)

    for k in range(EARLY):
        send_wm[k].start()
        send_wo[k].start()
    for copy in send_p:
        copy.start()
    for k in range(EARLY, chunks):
        send_wm[k].start()
    with jax.named_scope("build"):
        build_tiles()
    with jax.named_scope("first"):
        for k in range(EARLY):
            forward(k)
        local_k.wait()
        local_p.wait()
        for k in range(EARLY):
            local_w[k].wait()
            send_wo[k].wait_recv()
            send_wf[k].wait_recv()
        acc[...] = jnp.zeros_like(acc)
        each_tile(lambda t: add_product(slice(0, EARLY), 0, columns(t)))
    for i in range(PIECES):
        with jax.named_scope(f"piece#i={i}"):
            send_p[i].wait_recv()
            add_product(slice(0, EARLY), 1, slice(i * piece, (i + 1) * piece))

    def settle(k):
        for copy in send_p:
            copy.wait_send()
        for i in range(chunks):
            for copy in (send_wm[i], send_wo[i], send_wf[i], send_m[i], send_d[i], send_b[i]):
                copy.wait_send()
            for send in (send_z, send_e, send_g):
                each_peer(lambda step: send(i, step).wait_send())
        for i in range(chunks - 1):
            each_tile(lambda t: send_n(i, t, 0).wait_send())
            each_tile(lambda t: send_n(i, t, 1).wait_send())

    stages = {
        "forward": forward, "correlate": correlate, "reduce": reduce, "join": join, "mix": mix,
        "share": share_out, "expand": expand, "settle": settle,
    }
    for stage, k, t in schedule():
        with jax.named_scope(f"{stage}#k={k}#t={t}"):
            if stage == "far":
                far(k, t)
            elif stage == "near":
                near(k, t)
            else:
                stages[stage](k)
    with jax.named_scope("others"):
        for k in range(chunks - 1):
            each_tile(lambda t: send_o(k, t).wait())
        for k in range(chunks):
            each_tile(lambda t: write(k, t).wait())
    for side in range(2):
        each_tile(lambda t: send_n(chunks - 1, t, side).wait_send())
    with jax.named_scope("last"):
        each_tile(lambda t: send_o(chunks - 1, t).wait())


def square(nga, wavefunctions, projectors, kinetic_diag, species_index, coupling):
    bands, waves = wavefunctions.shape
    count = projectors.shape[0]
    atoms = species_index.shape[0]
    half, rows = waves // 2, bands // CHUNKS
    zn = nga // 2
    width, share = half // TILES, 4 * rows // zn
    bf16, f32 = jnp.bfloat16, jnp.float32
    dma = pltpu.SemaphoreType.DMA
    anywhere = pl.BlockSpec(memory_space=pl.ANY)
    return pl.pallas_call(
        functools.partial(kernel, nga),
        out_shape=jax.ShapeDtypeStruct((bands, waves), bf16),
        in_specs=[anywhere] * 5,
        out_specs=anywhere,
        scratch_shapes=[
            pltpu.VMEM((2, count, half), bf16),
            pltpu.VMEM((CHUNKS, 4, rows, half), bf16),
            pltpu.VMEM((EARLY, zn, share, 2 * count), f32),
            pltpu.VMEM((CHUNKS, zn, share, 2 * count), bf16),
            pltpu.VMEM((CHUNKS, share, 2 * count), f32),
            pltpu.VMEM((CHUNKS, zn - 1, share, 2 * count), bf16),
            pltpu.VMEM((CHUNKS, share, count), bf16),
            pltpu.VMEM((CHUNKS, share, count), bf16),
            pltpu.VMEM((CHUNKS, share, count), f32),
            pltpu.VMEM((CHUNKS, share, count), f32),
            pltpu.VMEM((CHUNKS, zn, share, 2 * count), bf16),
            pltpu.VMEM((CHUNKS, TILES, 2, rows, width), bf16),
            pltpu.VMEM((CHUNKS, TILES, 2, rows, width), bf16),
            pltpu.VMEM((CHUNKS, TILES, 2, rows, width), f32),
            pltpu.VMEM((CHUNKS, TILES, rows, width), bf16),
            pltpu.VMEM((CHUNKS, TILES, rows, width), bf16),
            pltpu.VMEM((1, half), f32),
            pltpu.VMEM((1, atoms), jnp.int32),
            pltpu.VMEM(coupling.shape, f32),
            pltpu.VMEM((count // LANES, LANES, LANES), f32),
            dma((4 + CHUNKS,)),
            dma((PIECES, 2)),
            dma((CHUNKS, 2)),
            dma((CHUNKS, 2)),
            dma((CHUNKS, 2)),
            dma((CHUNKS, zn - 1, 2)),
            dma((CHUNKS, 2)),
            dma((CHUNKS, 2)),
            dma((CHUNKS, 2)),
            dma((CHUNKS, zn - 1, 2)),
            dma((CHUNKS, zn - 1, 2)),
            dma((CHUNKS, TILES, 2, 2)),
            dma((CHUNKS, TILES, 2)),
            dma((CHUNKS, TILES)),
        ],
        compiler_params=pltpu.CompilerParams(
            collective_id=0, has_side_effects=True, vmem_limit_bytes=50 * 2**20
        ),
    )(
        wavefunctions, projectors, kinetic_diag.reshape(1, waves),
        species_index.reshape(1, atoms), coupling,
    )


def solution(mesh):
    in_specs = (P("band", "ga"), P("band", "ga"), P("ga"), P(), P())
    out_specs = P("band", "ga")
    nga = mesh.shape["ga"]
    fits = mesh.shape["band"] == 4 and nga % 8 == 0
    body = functools.partial(square, nga) if fits else local
    return jax.shard_map(body, mesh=mesh, in_specs=in_specs, out_specs=out_specs, check_vma=False)
```

```python
import functools

import jax
import jax.numpy as jnp
from jax import lax
from jax.experimental import pallas as pl
from jax.experimental.pallas import tpu as pltpu
from jax.sharding import PartitionSpec as P

CHUNKS = 4
TILES = 4
PIECES = 8
LANES = 128

NPA = 8


def apply_blocks(correlations, species_index, coupling, atom_start):
    rows = correlations.shape[0]
    count = correlations.shape[1] // NPA
    local_species = lax.dynamic_slice_in_dim(species_index, atom_start, count)
    onehot = (
        local_species[:, None] == jnp.arange(coupling.shape[0], dtype=jnp.int32)[None, :]
    ).astype(jnp.float32)
    blocks = jnp.einsum("as,sij->aij", onehot, coupling, precision=lax.Precision.HIGHEST)
    mixed = jnp.einsum(
        "baj,aij->bai",
        correlations.reshape(rows, count, NPA),
        blocks,
        precision=lax.Precision.HIGHEST,
    )
    return mixed.reshape(rows, count * NPA).astype(jnp.bfloat16)


def reduce_and_mix(partial_value, species_index, coupling, first_proj):
    total = lax.psum(partial_value.astype(jnp.bfloat16), "ga").astype(jnp.float32)
    return apply_blocks(total, species_index, coupling, first_proj // NPA)


def local(wavefunctions, projectors, kinetic_diag, species_index, coupling):
    proj_local = projectors.shape[0]
    band_index = lax.axis_index("band")
    partial_value = jnp.einsum(
        "bg,pg->bp",
        lax.all_gather(wavefunctions, "band", axis=0, tiled=True),
        projectors,
        preferred_element_type=jnp.float32,
    )
    mixed = reduce_and_mix(partial_value, species_index, coupling, band_index * proj_local)
    nonlocal_term = lax.psum_scatter(
        jnp.dot(mixed, projectors, preferred_element_type=jnp.float32).astype(jnp.bfloat16),
        "band",
        scatter_dimension=0,
        tiled=True,
    ).astype(jnp.float32)
    return (kinetic_diag[None, :] * wavefunctions.astype(jnp.float32) + nonlocal_term).astype(
        jnp.bfloat16
    )


EARLY = 2


def schedule():
    times = {
        "correlate": (0.3, 0.5, 16.5, 24.6),
        "forward": (None, None, 4.0, 9.5),
        "reduce": (7.5, 12.0, 29.3, 37.4),
        "join": (9.7, 15.0, 32.2, 40.0),
        "mix": (11.3, 21.2, 33.4, 41.2),
        "share": (14.4, 24.0, 36.0, 44.0),
        "expand": (21.5, 29.6, 42.0, 50.0),
        "settle": (57.0, None, None, None),
    }
    events = [
        (at, stage, k, 0)
        for stage, row in times.items()
        for k, at in enumerate(row)
        if at is not None
    ]
    for k, (first, step) in enumerate(((29.5, 0.02), (36.5, 1.2), (50.5, 1.2), (62.0, 1.0))):
        events += [(first + step * t, "far", k, t) for t in range(TILES)]
    for k, first in enumerate((44.2, 52.6, 58.0, 70.0)):
        events += [(first + 0.05 * t, "near", k, t) for t in range(TILES)]
    return [event[1:] for event in sorted(events)]


def kernel(
    nga, wf, pj, kin_hbm, species_hbm, coupling_hbm, out,
    proj, wave, acc, csend, keep, parts, msend, mrecv, dsend, drecv, mixed,
    nsend, nrecv, own, nfull, ready, kin, species, coupling, tiles,
    s_send, s_loc, s_p, s_wm, s_wo, s_m, s_d, s_b, s_z, s_e, s_far, s_near, s_out,
):
    chunks, _, rows, half = wave.shape
    _, zn, share, both = csend.shape
    count = both // 2
    width = nsend.shape[-1]
    piece = half // PIECES
    quarter = zn // 4
    band, me = lax.axis_index("band"), lax.axis_index("ga")
    core, z, y, x = me % 2, me // 2, band // 2, band % 2
    across_x, across_y, diag = y * 2 + 1 - x, (1 - y) * 2 + x, 3 - band
    m = (1 - core) * y + core * x
    m_nbr = (1 - core) * across_y + core * across_x
    o_nbr = (1 - core) * across_x + core * across_y
    here = pl.multiple_of(m * half, LANES)
    there = pl.multiple_of((1 - m) * half, LANES)
    to_m, to_o, to_twin = {"band": m_nbr}, {"band": o_nbr}, {"ga": z * 2 + 1 - core}

    def remote(src, dst, sent, received, device):
        return pltpu.make_async_remote_copy(
            src_ref=src, dst_ref=dst, send_sem=s_send.at[sent], recv_sem=received,
            device_id=device, device_id_type=pl.DeviceIdType.MESH,
        )

    def span(k):
        return pl.ds(k * rows, rows)

    def peer(step):
        return (z + 1 + step) % zn

    def to_peer(step):
        return {"ga": peer(step) * 2 + core}

    local_p = pltpu.make_async_copy(pj.at[:, pl.ds(here, half)], proj.at[0], s_loc.at[0])
    local_k = pltpu.make_async_copy(kin_hbm.at[:, pl.ds(here, half)], kin, s_loc.at[1])
    local_s = pltpu.make_async_copy(species_hbm, species, s_loc.at[2])
    local_c = pltpu.make_async_copy(coupling_hbm, coupling, s_loc.at[3])
    local_w = [
        pltpu.make_async_copy(wf.at[span(k), pl.ds(here, half)], wave.at[k, band], s_loc.at[4])
        for k in range(chunks)
    ]
    send_p = [
        remote(
            pj.at[:, pl.ds(pl.multiple_of(there + i * piece, LANES), piece)],
            proj.at[1, :, pl.ds(i * piece, piece)], 0, s_p.at[i], to_m,
        )
        for i in range(PIECES)
    ]
    send_wm = [
        remote(wf.at[span(k), pl.ds(there, half)], wave.at[k, band], 1, s_wm.at[k], to_m)
        for k in range(chunks)
    ]
    send_wo = [
        remote(
            wf.at[span(k), pl.ds(here, half)], wave.at[k, band], 2,
            s_wo.at[max(k - EARLY + 1, 0)], to_o,
        )
        for k in range(chunks)
    ]
    send_wf = [
        remote(
            wave.at[k, m_nbr], wave.at[k, m_nbr], 3, s_wo.at[max(k - EARLY + 1, 0)], to_o
        )
        for k in range(chunks)
    ]
    send_m = [remote(msend.at[k], mrecv.at[k], 4, s_m.at[k], to_m) for k in range(chunks)]
    send_d = [remote(dsend.at[k], drecv.at[k], 5, s_d.at[k], to_twin) for k in range(chunks)]
    send_b = [
        remote(mixed.at[k, z, :, :count], mixed.at[k, z, :, count:], 6, s_b.at[k], to_m)
        for k in range(chunks)
    ]

    def send_z(k, step):
        return remote(csend.at[k, peer(step)], parts.at[k, step], 7, s_z.at[k], to_peer(step))

    def send_e(k, step):
        block = mixed.at[k, z, :, :count]
        return remote(block, block, 8, s_e.at[k], to_peer(step))

    def send_g(k, step):
        block = mixed.at[k, z, :, count:]
        return remote(block, block, 8, s_e.at[k], to_peer(step))

    def send_n(k, t, side):
        if side:
            received = s_far.at[k, t]
        else:
            received = s_near.at[k + t if k == chunks - 1 else k]
        return remote(nsend.at[k, t, side], nrecv.at[k, t, side], 9 + side, received, to_o)

    def place(k, t):
        return out.at[span(k), pl.ds(pl.multiple_of(here + t * width, LANES), width)]

    def send_o(k, t):
        return remote(nfull.at[k, t], place(k, t), 11, s_out.at[0], to_m)

    def write(k, t):
        return pltpu.make_async_copy(ready.at[k, t], place(k, t), s_out.at[1])

    def arrived(ref, semaphore):
        pltpu.make_async_copy(ref, ref, semaphore).wait()

    def each_peer(body):
        def step(i, carry):
            body(i)
            return carry

        lax.fori_loop(0, zn - 1, step, 0)

    def each_tile(body):
        def step(i, carry):
            body(i)
            return carry

        lax.fori_loop(0, TILES, step, 0)

    def columns(t):
        return pl.ds(pl.multiple_of(t * width, LANES), width)

    def add_product(chunk, slot, cols):
        product = lax.dot_general(
            wave[chunk, :, :, cols].reshape(-1, proj[slot, :, cols].shape[-1]),
            proj[slot, :, cols],
            (((1,), (1,)), ((), ())),
            preferred_element_type=jnp.float32,
        )
        product = product.reshape(-1, zn, share, count)
        acc[: product.shape[0], :, :, slot * count : (slot + 1) * count] += product

    def build_tiles():
        kinds, npa = coupling.shape[0], coupling.shape[1]
        atoms = species.shape[1]
        local_s.wait()
        local_c.wait()
        first = band * (count // npa)
        atom = lax.broadcasted_iota(jnp.int32, (atoms, count), 0)
        column = lax.broadcasted_iota(jnp.int32, (atoms, count), 1)
        spread = (atom == first + column // npa).astype(jnp.float32)
        kind = lax.broadcasted_iota(jnp.int32, (8, atoms), 0)
        onehot = (kind == species[...]).astype(jnp.float32)
        chosen = jnp.dot(
            onehot, spread, preferred_element_type=jnp.float32, precision=lax.Precision.HIGHEST
        )
        row = lax.broadcasted_iota(jnp.int32, (LANES, npa), 0)
        index = lax.broadcasted_iota(jnp.int32, (LANES, npa), 1)
        repeat = (row % npa == index).astype(jnp.float32)
        blocks = []
        for s in range(kinds):
            tall = lax.dot_general(
                repeat, coupling[s], (((1,), (1,)), ((), ())),
                preferred_element_type=jnp.float32, precision=lax.Precision.HIGHEST,
            )
            blocks.append(
                lax.dot_general(
                    tall, repeat, (((1,), (1,)), ((), ())),
                    preferred_element_type=jnp.float32, precision=lax.Precision.HIGHEST,
                )
            )
        atom_row = lax.broadcasted_iota(jnp.int32, (LANES, LANES), 0) // npa
        atom_col = lax.broadcasted_iota(jnp.int32, (LANES, LANES), 1) // npa
        same = atom_row == atom_col
        for t in range(tiles.shape[0]):
            value = jnp.zeros((LANES, LANES), jnp.float32)
            for s in range(kinds):
                here_kind = chosen[s : s + 1, t * LANES : (t + 1) * LANES]
                value = jnp.where(here_kind > 0.5, blocks[s], value)
            tiles[t] = jnp.where(same, value, 0.0)

    def forward(k):
        send_wm[k].wait_recv()
        if k == EARLY:
            send_wo[k].start()
        send_wf[k].start()
        if k == EARLY:
            for later in range(EARLY + 1, chunks):
                send_wo[later].start()

    def correlate(k):
        place = k
        if k >= EARLY:
            place = 0
            arrived(wave.at[k, pl.ds(0, 2)], s_wo.at[k - EARLY + 1])
            acc[0] = jnp.zeros_like(acc[0])

            def tile(t):
                add_product(slice(k, k + 1), 0, columns(t))
                add_product(slice(k, k + 1), 1, columns(t))

            each_tile(tile)
        csend[k] = acc[place].astype(jnp.bfloat16)
        each_peer(lambda step: send_z(k, step).start())
        keep[k] = acc[place, z]

    def reduce(k):
        arrived(parts.at[k], s_z.at[k])
        total = keep[k]
        for step in range(zn - 1):
            total = total + parts[k, step].astype(jnp.float32)
        msend[k] = total[:, count:].astype(jnp.bfloat16)
        send_m[k].start()
        dsend[k] = total[:, :count]

    def join(k):
        send_m[k].wait_recv()
        dsend[k] = dsend[k] + mrecv[k].astype(jnp.float32)
        send_d[k].start()

    def mix(k):
        send_d[k].wait_recv()
        total = dsend[k] + drecv[k]
        for t in range(tiles.shape[0]):
            cols = slice(t * LANES, (t + 1) * LANES)
            mixed[k, z, :, cols] = jnp.dot(
                total[:, cols], tiles[t],
                preferred_element_type=jnp.float32, precision=lax.Precision.HIGHEST,
            ).astype(jnp.bfloat16)
        send_b[k].start()
        each_peer(lambda step: send_e(k, step).start())

    def share_out(k):
        send_b[k].wait_recv()
        each_peer(lambda step: send_g(k, step).start())

    def expand(k):
        arrived(parts.at[k], s_e.at[k])

        def tile(t):
            cols = columns(t)
            picks = [
                mixed[k, pl.ds(b * quarter, quarter)].reshape(rows, both)
                for b in (o_nbr, diag, band, m_nbr)
            ]
            value = jnp.dot(
                jnp.concatenate(picks, axis=0), proj[:, :, cols].reshape(both, width),
                preferred_element_type=jnp.float32,
            ).reshape(4, rows, width)
            nsend[k, t] = value[:2].astype(jnp.bfloat16)
            send_n(k, t, 1).start()
            own[k, t] = value[2:]

        each_tile(tile)
        each_tile(lambda t: send_n(k, t, 0).start())

    def complete(k, t, side, owner):
        cols = columns(t)
        kinetic = kin[:, cols] * wave[k, owner, :, cols].astype(jnp.float32)
        total = own[k, t, side] + nrecv[k, t, side].astype(jnp.float32)
        return (kinetic + total).astype(jnp.bfloat16)

    def far(k, t):
        send_n(k, t, 1).wait_recv()
        nfull[k, t] = complete(k, t, 1, m_nbr)
        send_o(k, t).start()

    def near(k, t):
        if k == chunks - 1:
            send_n(k, t, 0).wait_recv()
        elif t == 0:
            arrived(nrecv.at[k, :, 0], s_near.at[k])
        ready[k, t] = complete(k, t, 0, band)
        write(k, t).start()

    barrier = pltpu.get_barrier_semaphore()
    for device in (to_m, to_o, to_twin):
        pl.semaphore_signal(
            barrier, inc=1, device_id=device, device_id_type=pl.DeviceIdType.MESH
        )
    each_peer(
        lambda step: pl.semaphore_signal(
            barrier, inc=1, device_id=to_peer(step), device_id_type=pl.DeviceIdType.MESH
        )
    )
    local_p.start()
    for copy in local_w:
        copy.start()
    local_s.start()
    local_c.start()
    local_k.start()
    pl.semaphore_wait(barrier, zn + 2)

    for k in range(EARLY):
        send_wm[k].start()
        send_wo[k].start()
    for copy in send_p:
        copy.start()
    for k in range(EARLY, chunks):
        send_wm[k].start()
    with jax.named_scope("build"):
        build_tiles()
    with jax.named_scope("first"):
        for k in range(EARLY):
            forward(k)
        local_k.wait()
        local_p.wait()
        arrived(wave.at[:, 0], s_loc.at[4])
        arrived(wave.at[pl.ds(0, EARLY), pl.ds(0, 2)], s_wo.at[0])
        acc[...] = jnp.zeros_like(acc)
        each_tile(lambda t: add_product(slice(0, EARLY), 0, columns(t)))
    for i in range(PIECES):
        with jax.named_scope(f"piece#i={i}"):
            send_p[i].wait_recv()
            add_product(slice(0, EARLY), 1, slice(i * piece, (i + 1) * piece))

    def settle(k):
        sent = (
            proj.at[1], wave.at[:, 0], wave.at[:, 0], wave.at[:, 0], mrecv, drecv, msend, parts, parts
        )
        for kind, ref in enumerate(sent):
            arrived(ref, s_send.at[kind])

    stages = {
        "forward": forward, "correlate": correlate, "reduce": reduce, "join": join, "mix": mix,
        "share": share_out, "expand": expand, "settle": settle,
    }
    for stage, k, t in schedule():
        with jax.named_scope(f"{stage}#k={k}#t={t}"):
            if stage == "far":
                far(k, t)
            elif stage == "near":
                near(k, t)
            else:
                stages[stage](k)
    with jax.named_scope("others"):
        arrived(ready, s_out.at[1])
        arrived(nsend.at[:, :, 0], s_send.at[9])
        arrived(nsend.at[:, :, 1], s_send.at[10])
        arrived(nfull, s_send.at[11])
    with jax.named_scope("last"):
        arrived(nfull, s_out.at[0])


def square(nga, wavefunctions, projectors, kinetic_diag, species_index, coupling):
    bands, waves = wavefunctions.shape
    count = projectors.shape[0]
    atoms = species_index.shape[0]
    half, rows = waves // 2, bands // CHUNKS
    zn = nga // 2
    width, share = half // TILES, 4 * rows // zn
    bf16, f32 = jnp.bfloat16, jnp.float32
    dma = pltpu.SemaphoreType.DMA
    anywhere = pl.BlockSpec(memory_space=pl.ANY)
    return pl.pallas_call(
        functools.partial(kernel, nga),
        out_shape=jax.ShapeDtypeStruct((bands, waves), bf16),
        in_specs=[anywhere] * 5,
        out_specs=anywhere,
        scratch_shapes=[
            pltpu.VMEM((2, count, half), bf16),
            pltpu.VMEM((CHUNKS, 4, rows, half), bf16),
            pltpu.VMEM((EARLY, zn, share, 2 * count), f32),
            pltpu.VMEM((CHUNKS, zn, share, 2 * count), bf16),
            pltpu.VMEM((CHUNKS, share, 2 * count), f32),
            pltpu.VMEM((CHUNKS, zn - 1, share, 2 * count), bf16),
            pltpu.VMEM((CHUNKS, share, count), bf16),
            pltpu.VMEM((CHUNKS, share, count), bf16),
            pltpu.VMEM((CHUNKS, share, count), f32),
            pltpu.VMEM((CHUNKS, share, count), f32),
            pltpu.VMEM((CHUNKS, zn, share, 2 * count), bf16),
            pltpu.VMEM((CHUNKS, TILES, 2, rows, width), bf16),
            pltpu.VMEM((CHUNKS, TILES, 2, rows, width), bf16),
            pltpu.VMEM((CHUNKS, TILES, 2, rows, width), f32),
            pltpu.VMEM((CHUNKS, TILES, rows, width), bf16),
            pltpu.VMEM((CHUNKS, TILES, rows, width), bf16),
            pltpu.VMEM((1, half), f32),
            pltpu.VMEM((1, atoms), jnp.int32),
            pltpu.VMEM(coupling.shape, f32),
            pltpu.VMEM((count // LANES, LANES, LANES), f32),
            dma((12,)),
            dma((5,)),
            dma((PIECES,)),
            dma((CHUNKS,)),
            dma((CHUNKS - EARLY + 1,)),
            dma((CHUNKS,)),
            dma((CHUNKS,)),
            dma((CHUNKS,)),
            dma((CHUNKS,)),
            dma((CHUNKS,)),
            dma((CHUNKS, TILES)),
            dma((CHUNKS + TILES - 1,)),
            dma((2,)),
        ],
        compiler_params=pltpu.CompilerParams(
            collective_id=0, has_side_effects=True, vmem_limit_bytes=50 * 2**20
        ),
    )(
        wavefunctions, projectors, kinetic_diag.reshape(1, waves),
        species_index.reshape(1, atoms), coupling,
    )


def solution(mesh):
    in_specs = (P("band", "ga"), P("band", "ga"), P("ga"), P(), P())
    out_specs = P("band", "ga")
    nga = mesh.shape["ga"]
    fits = mesh.shape["band"] == 4 and nga % 8 == 0
    body = functools.partial(square, nga) if fits else local
    return jax.shard_map(body, mesh=mesh, in_specs=in_specs, out_specs=out_specs, check_vma=False)
```

```python
import functools

import jax
import jax.numpy as jnp
from jax import lax
from jax.experimental import pallas as pl
from jax.experimental.pallas import tpu as pltpu
from jax.sharding import PartitionSpec as P

CHUNKS = 4
TILES = 4
PIECES = 8
LANES = 128

NPA = 8


def apply_blocks(correlations, species_index, coupling, atom_start):
    rows = correlations.shape[0]
    count = correlations.shape[1] // NPA
    local_species = lax.dynamic_slice_in_dim(species_index, atom_start, count)
    onehot = (
        local_species[:, None] == jnp.arange(coupling.shape[0], dtype=jnp.int32)[None, :]
    ).astype(jnp.float32)
    blocks = jnp.einsum("as,sij->aij", onehot, coupling, precision=lax.Precision.HIGHEST)
    mixed = jnp.einsum(
        "baj,aij->bai",
        correlations.reshape(rows, count, NPA),
        blocks,
        precision=lax.Precision.HIGHEST,
    )
    return mixed.reshape(rows, count * NPA).astype(jnp.bfloat16)


def reduce_and_mix(partial_value, species_index, coupling, first_proj):
    total = lax.psum(partial_value.astype(jnp.bfloat16), "ga").astype(jnp.float32)
    return apply_blocks(total, species_index, coupling, first_proj // NPA)


def local(wavefunctions, projectors, kinetic_diag, species_index, coupling):
    proj_local = projectors.shape[0]
    band_index = lax.axis_index("band")
    partial_value = jnp.einsum(
        "bg,pg->bp",
        lax.all_gather(wavefunctions, "band", axis=0, tiled=True),
        projectors,
        preferred_element_type=jnp.float32,
    )
    mixed = reduce_and_mix(partial_value, species_index, coupling, band_index * proj_local)
    nonlocal_term = lax.psum_scatter(
        jnp.dot(mixed, projectors, preferred_element_type=jnp.float32).astype(jnp.bfloat16),
        "band",
        scatter_dimension=0,
        tiled=True,
    ).astype(jnp.float32)
    return (kinetic_diag[None, :] * wavefunctions.astype(jnp.float32) + nonlocal_term).astype(
        jnp.bfloat16
    )


EARLY = 2


def schedule():
    times = {
        "correlate": (0.3, 0.5, 16.6, 24.8),
        "forward": (None, None, 4.0, 9.5),
        "reduce": (7.5, 12.0, 29.7, 38.0),
        "join": (9.7, 15.0, 30.0, 39.5),
        "mix": (11.3, 16.3, 31.2, 40.7),
        "share": (14.4, 22.1, 36.1, 43.2),
        "expand": (22.2, 31.3, 43.5, 50.0),
        "settle": (57.0, None, None, None),
    }
    events = [
        (at, stage, k, 0)
        for stage, row in times.items()
        for k, at in enumerate(row)
        if at is not None
    ]
    for k, row in enumerate(((29.8, 29.82, 36.02, 36.04), (40.9, 40.92, 46.0, 46.1), (50.5, 51.5, 52.5, 53.5), (62.0, 63.0, 64.0, 65.0))):
        events += [(at, "far", k, t) for t, at in enumerate(row)]
    for k, first in enumerate((46.5, 52.6, 58.0, 70.0)):
        events += [(first + 0.05 * t, "near", k, t) for t in range(TILES)]
    return [event[1:] for event in sorted(events)]


def kernel(
    nga, wf, pj, kin_hbm, species_hbm, coupling_hbm, out,
    proj, wave, acc, csend, keep, parts, msend, mrecv, dsend, drecv, mixed,
    nsend, nrecv, own, nfull, ready, kin, species, coupling, tiles,
    s_send, s_loc, s_p, s_wm, s_wo, s_m, s_d, s_b, s_z, s_e, s_far, s_near, s_out, s_token,
):
    chunks, _, rows, half = wave.shape
    _, zn, share, both = csend.shape
    count = both // 2
    width = nsend.shape[-1]
    piece = half // PIECES
    quarter = zn // 4
    band, me = lax.axis_index("band"), lax.axis_index("ga")
    core, z, y, x = me % 2, me // 2, band // 2, band % 2
    across_x, across_y, diag = y * 2 + 1 - x, (1 - y) * 2 + x, 3 - band
    m = (1 - core) * y + core * x
    m_nbr = (1 - core) * across_y + core * across_x
    o_nbr = (1 - core) * across_x + core * across_y
    here = pl.multiple_of(m * half, LANES)
    there = pl.multiple_of((1 - m) * half, LANES)
    to_m, to_o, to_twin = {"band": m_nbr}, {"band": o_nbr}, {"ga": z * 2 + 1 - core}

    def remote(src, dst, sent, received, device):
        return pltpu.make_async_remote_copy(
            src_ref=src, dst_ref=dst, send_sem=s_send.at[sent], recv_sem=received,
            device_id=device, device_id_type=pl.DeviceIdType.MESH,
        )

    def span(k):
        return pl.ds(k * rows, rows)

    def peer(step):
        return (z + 1 + step) % zn

    def to_peer(step):
        return {"ga": peer(step) * 2 + core}

    local_p = pltpu.make_async_copy(pj.at[:, pl.ds(here, half)], proj.at[0], s_loc.at[0])
    local_k = pltpu.make_async_copy(kin_hbm.at[:, pl.ds(here, half)], kin, s_loc.at[1])
    local_s = pltpu.make_async_copy(species_hbm, species, s_loc.at[2])
    local_c = pltpu.make_async_copy(coupling_hbm, coupling, s_loc.at[4])
    local_w = [
        pltpu.make_async_copy(wf.at[span(k), pl.ds(here, half)], wave.at[k, band], s_loc.at[3])
        for k in range(chunks)
    ]
    send_p = [
        remote(
            pj.at[:, pl.ds(pl.multiple_of(there + i * piece, LANES), piece)],
            proj.at[1, :, pl.ds(i * piece, piece)], 0, s_p.at[i], to_m,
        )
        for i in range(PIECES)
    ]
    send_wm = [
        remote(wf.at[span(k), pl.ds(there, half)], wave.at[k, band], 1, s_wm.at[k], to_m)
        for k in range(chunks)
    ]
    send_wo = [
        remote(
            wf.at[span(k), pl.ds(here, half)], wave.at[k, band], 2,
            s_wo.at[max(k - EARLY + 1, 0)], to_o,
        )
        for k in range(chunks)
    ]
    send_wf = [
        remote(
            wave.at[k, m_nbr], wave.at[k, m_nbr], 3, s_wo.at[max(k - EARLY + 1, 0)], to_o
        )
        for k in range(chunks)
    ]
    send_m = [remote(msend.at[k], mrecv.at[k], 4, s_m.at[k], to_m) for k in range(chunks)]
    send_d = [remote(dsend.at[k], drecv.at[k], 5, s_d.at[k], to_twin) for k in range(chunks)]
    send_b = [
        remote(mixed.at[k, z, :, :count], mixed.at[k, z, :, count:], 6, s_b.at[k], to_m)
        for k in range(chunks)
    ]

    def send_z(k, step):
        return remote(csend.at[k, peer(step)], parts.at[k, step], 7, s_z.at[k], to_peer(step))

    def send_e(k, step):
        block = mixed.at[k, z, :, :count]
        return remote(block, block, 8, s_e.at[k], to_peer(step))

    def send_g(k, step):
        block = mixed.at[k, z, :, count:]
        return remote(block, block, 8, s_e.at[k], to_peer(step))

    def send_near(k):
        return remote(nsend.at[k, 0], nrecv.at[k, 0], 9, s_near.at[k], to_o)

    def send_n(k, t, side):
        received = s_far.at[k, t] if side else s_near.at[k + t]
        return remote(nsend.at[k, side, t], nrecv.at[k, side, t], 9, received, to_o)

    def place(k, t):
        return out.at[span(k), pl.ds(pl.multiple_of(here + t * width, LANES), width)]

    def send_o(k, t):
        return remote(nfull.at[k, t], place(k, t), 10, s_out.at[0], to_m)

    def write(k, t):
        return pltpu.make_async_copy(ready.at[k, t], place(k, t), s_out.at[1])

    def arrived(ref, semaphore):
        pltpu.make_async_copy(ref, ref, semaphore).wait()

    def each_peer(body):
        def step(i, carry):
            body(i)
            return carry

        lax.fori_loop(0, zn - 1, step, 0)

    def each_tile(body):
        def step(i, carry):
            body(i)
            return carry

        lax.fori_loop(0, TILES, step, 0)

    def columns(t):
        return pl.ds(pl.multiple_of(t * width, LANES), width)

    def add_product(chunk, slot, cols):
        product = lax.dot_general(
            wave[chunk, :, :, cols].reshape(-1, proj[slot, :, cols].shape[-1]),
            proj[slot, :, cols],
            (((1,), (1,)), ((), ())),
            preferred_element_type=jnp.float32,
        )
        product = product.reshape(-1, zn, share, count)
        acc[: product.shape[0], :, :, slot * count : (slot + 1) * count] += product

    def build_tiles():
        kinds, npa = coupling.shape[0], coupling.shape[1]
        atoms = species.shape[1]
        local_s.wait()
        local_c.wait()
        first = band * (count // npa)
        atom = lax.broadcasted_iota(jnp.int32, (atoms, count), 0)
        column = lax.broadcasted_iota(jnp.int32, (atoms, count), 1)
        spread = (atom == first + column // npa).astype(jnp.float32)
        kind = lax.broadcasted_iota(jnp.int32, (8, atoms), 0)
        onehot = (kind == species[...]).astype(jnp.float32)
        chosen = jnp.dot(
            onehot, spread, preferred_element_type=jnp.float32, precision=lax.Precision.HIGHEST
        )
        row = lax.broadcasted_iota(jnp.int32, (LANES, npa), 0)
        index = lax.broadcasted_iota(jnp.int32, (LANES, npa), 1)
        repeat = (row % npa == index).astype(jnp.float32)
        blocks = []
        for s in range(kinds):
            tall = lax.dot_general(
                repeat, coupling[s], (((1,), (1,)), ((), ())),
                preferred_element_type=jnp.float32, precision=lax.Precision.HIGHEST,
            )
            blocks.append(
                lax.dot_general(
                    tall, repeat, (((1,), (1,)), ((), ())),
                    preferred_element_type=jnp.float32, precision=lax.Precision.HIGHEST,
                )
            )
        atom_row = lax.broadcasted_iota(jnp.int32, (LANES, LANES), 0) // npa
        atom_col = lax.broadcasted_iota(jnp.int32, (LANES, LANES), 1) // npa
        same = atom_row == atom_col
        for t in range(tiles.shape[0]):
            value = jnp.zeros((LANES, LANES), jnp.float32)
            for s in range(kinds):
                here_kind = chosen[s : s + 1, t * LANES : (t + 1) * LANES]
                value = jnp.where(here_kind > 0.5, blocks[s], value)
            tiles[t] = jnp.where(same, value, 0.0)

    def forward(k):
        send_wm[k].wait_recv()
        if k == EARLY:
            send_wo[k].start()
        send_wf[k].start()
        if k == EARLY:
            for later in range(EARLY + 1, chunks):
                send_wo[later].start()

    def correlate(k):
        place = k
        if k >= EARLY:
            place = 0
            arrived(wave.at[k, pl.ds(0, 2)], s_wo.at[k - EARLY + 1])
            acc[0] = jnp.zeros_like(acc[0])

            def tile(t):
                add_product(slice(k, k + 1), 0, columns(t))
                add_product(slice(k, k + 1), 1, columns(t))

            each_tile(tile)
        csend[k] = acc[place].astype(jnp.bfloat16)
        each_peer(lambda step: send_z(k, step).start())
        keep[k] = acc[place, z]

    def reduce(k):
        arrived(parts.at[k], s_z.at[k])
        total = keep[k]
        for step in range(zn - 1):
            total = total + parts[k, step].astype(jnp.float32)
        msend[k] = total[:, count:].astype(jnp.bfloat16)
        send_m[k].start()
        dsend[k] = total[:, :count]

    def join(k):
        send_m[k].wait_recv()
        dsend[k] = dsend[k] + mrecv[k].astype(jnp.float32)
        send_d[k].start()

    def mix(k):
        send_d[k].wait_recv()
        total = dsend[k] + drecv[k]
        for t in range(tiles.shape[0]):
            cols = slice(t * LANES, (t + 1) * LANES)
            mixed[k, z, :, cols] = jnp.dot(
                total[:, cols], tiles[t],
                preferred_element_type=jnp.float32, precision=lax.Precision.HIGHEST,
            ).astype(jnp.bfloat16)
        send_b[k].start()
        each_peer(lambda step: send_e(k, step).start())

    def share_out(k):
        send_b[k].wait_recv()
        each_peer(lambda step: send_g(k, step).start())

    def expand(k):
        arrived(parts.at[k], s_e.at[k])

        def tile(t):
            cols = columns(t)
            picks = [
                mixed[k, pl.ds(b * quarter, quarter)].reshape(rows, both)
                for b in (o_nbr, diag, band, m_nbr)
            ]
            value = jnp.dot(
                jnp.concatenate(picks, axis=0), proj[:, :, cols].reshape(both, width),
                preferred_element_type=jnp.float32,
            ).reshape(4, rows, width)
            nsend[k, :, t] = value[:2].astype(jnp.bfloat16)
            send_n(k, t, 1).start()
            own[k, t] = value[2:]

        each_tile(tile)
        if k == chunks - 1:
            each_tile(lambda t: send_n(k, t, 0).start())
        else:
            send_near(k).start()

    def complete(k, t, side, owner):
        cols = columns(t)
        kinetic = kin[:, cols] * wave[k, owner, :, cols].astype(jnp.float32)
        total = own[k, t, side] + nrecv[k, side, t].astype(jnp.float32)
        return (kinetic + total).astype(jnp.bfloat16)

    def far(k, t):
        send_n(k, t, 1).wait_recv()
        nfull[k, t] = complete(k, t, 1, m_nbr)
        send_o(k, t).start()

    def near(k, t):
        if k == chunks - 1:
            send_n(k, t, 0).wait_recv()
        elif t == 0:
            send_near(k).wait_recv()
        ready[k, t] = complete(k, t, 0, band)
        write(k, t).start()

    barrier = pltpu.get_barrier_semaphore()

    def greet(semaphore, device):
        pl.semaphore_signal(
            semaphore, inc=1, device_id=device, device_id_type=pl.DeviceIdType.MESH
        )

    above, below = {"ga": (z + 1) * 2 + core}, {"ga": (z - 1) * 2 + core}
    has_above, has_below = z < zn - 1, z > 0
    for device in (to_m, to_o, to_twin):
        greet(barrier, device)
    pl.when(has_above)(lambda: greet(barrier, above))
    pl.when(has_below)(lambda: greet(barrier, below))
    local_p.start()
    for copy in local_w:
        copy.start()
    local_s.start()
    local_c.start()
    local_k.start()
    pl.semaphore_wait(barrier, 3 + has_above.astype(jnp.int32) + has_below.astype(jnp.int32))

    for k in range(EARLY):
        send_wm[k].start()
        send_wo[k].start()
    for copy in send_p:
        copy.start()
    for k in range(EARLY, chunks):
        send_wm[k].start()
    with jax.named_scope("tokens"):
        pl.when(has_below)(lambda: pl.semaphore_wait(s_token.at[0], 1))
        pl.when(has_above)(lambda: greet(s_token.at[0], above))
        pl.when(has_above)(lambda: pl.semaphore_wait(s_token.at[1], 1))
        pl.when(has_below)(lambda: greet(s_token.at[1], below))
    with jax.named_scope("build"):
        build_tiles()
    with jax.named_scope("first"):
        for k in range(EARLY):
            forward(k)
        local_k.wait()
        local_p.wait()
        arrived(wave.at[:, 0], s_loc.at[3])
        arrived(wave.at[pl.ds(0, EARLY), pl.ds(0, 2)], s_wo.at[0])
        acc[...] = jnp.zeros_like(acc)
        each_tile(lambda t: add_product(slice(0, EARLY), 0, columns(t)))
    for i in range(PIECES):
        with jax.named_scope(f"piece#i={i}"):
            send_p[i].wait_recv()
            add_product(slice(0, EARLY), 1, slice(i * piece, (i + 1) * piece))

    def settle(k):
        sent = (
            proj.at[1], wave.at[:, 0], wave.at[:, 0], wave.at[:, 0], mrecv, drecv, msend, parts, parts
        )
        for kind, ref in enumerate(sent):
            arrived(ref, s_send.at[kind])

    stages = {
        "forward": forward, "correlate": correlate, "reduce": reduce, "join": join, "mix": mix,
        "share": share_out, "expand": expand, "settle": settle,
    }
    for stage, k, t in schedule():
        with jax.named_scope(f"{stage}#k={k}#t={t}"):
            if stage == "far":
                far(k, t)
            elif stage == "near":
                near(k, t)
            else:
                stages[stage](k)
    with jax.named_scope("others"):
        arrived(ready, s_out.at[1])
        arrived(nsend, s_send.at[9])
        arrived(nfull, s_send.at[10])
    with jax.named_scope("last"):
        arrived(nfull, s_out.at[0])


def square(nga, wavefunctions, projectors, kinetic_diag, species_index, coupling):
    bands, waves = wavefunctions.shape
    count = projectors.shape[0]
    atoms = species_index.shape[0]
    half, rows = waves // 2, bands // CHUNKS
    zn = nga // 2
    width, share = half // TILES, 4 * rows // zn
    bf16, f32 = jnp.bfloat16, jnp.float32
    dma = pltpu.SemaphoreType.DMA
    anywhere = pl.BlockSpec(memory_space=pl.ANY)
    return pl.pallas_call(
        functools.partial(kernel, nga),
        out_shape=jax.ShapeDtypeStruct((bands, waves), bf16),
        in_specs=[anywhere] * 5,
        out_specs=anywhere,
        scratch_shapes=[
            pltpu.VMEM((2, count, half), bf16),
            pltpu.VMEM((CHUNKS, 4, rows, half), bf16),
            pltpu.VMEM((EARLY, zn, share, 2 * count), f32),
            pltpu.VMEM((CHUNKS, zn, share, 2 * count), bf16),
            pltpu.VMEM((CHUNKS, share, 2 * count), f32),
            pltpu.VMEM((CHUNKS, zn - 1, share, 2 * count), bf16),
            pltpu.VMEM((CHUNKS, share, count), bf16),
            pltpu.VMEM((CHUNKS, share, count), bf16),
            pltpu.VMEM((CHUNKS, share, count), f32),
            pltpu.VMEM((CHUNKS, share, count), f32),
            pltpu.VMEM((CHUNKS, zn, share, 2 * count), bf16),
            pltpu.VMEM((CHUNKS, 2, TILES, rows, width), bf16),
            pltpu.VMEM((CHUNKS, 2, TILES, rows, width), bf16),
            pltpu.VMEM((CHUNKS, TILES, 2, rows, width), f32),
            pltpu.VMEM((CHUNKS, TILES, rows, width), bf16),
            pltpu.VMEM((CHUNKS, TILES, rows, width), bf16),
            pltpu.VMEM((1, half), f32),
            pltpu.VMEM((1, atoms), jnp.int32),
            pltpu.VMEM(coupling.shape, f32),
            pltpu.VMEM((count // LANES, LANES, LANES), f32),
            dma((11,)),
            dma((5,)),
            dma((PIECES,)),
            dma((CHUNKS,)),
            dma((CHUNKS - EARLY + 1,)),
            dma((CHUNKS,)),
            dma((CHUNKS,)),
            dma((CHUNKS,)),
            dma((CHUNKS,)),
            dma((CHUNKS,)),
            dma((CHUNKS, TILES)),
            dma((CHUNKS + TILES - 1,)),
            dma((2,)),
            pltpu.SemaphoreType.REGULAR((2,)),
        ],
        compiler_params=pltpu.CompilerParams(
            collective_id=0, has_side_effects=True, vmem_limit_bytes=50 * 2**20
        ),
    )(
        wavefunctions, projectors, kinetic_diag.reshape(1, waves),
        species_index.reshape(1, atoms), coupling,
    )


def solution(mesh):
    in_specs = (P("band", "ga"), P("band", "ga"), P("ga"), P(), P())
    out_specs = P("band", "ga")
    nga = mesh.shape["ga"]
    fits = mesh.shape["band"] == 4 and nga % 8 == 0
    body = functools.partial(square, nga) if fits else local
    return jax.shard_map(body, mesh=mesh, in_specs=in_specs, out_specs=out_specs, check_vma=False)
```

```python
import functools

import jax
import jax.numpy as jnp
from jax import lax
from jax.experimental import pallas as pl
from jax.experimental.pallas import tpu as pltpu
from jax.sharding import PartitionSpec as P

CHUNKS = 4
TILES = 4
PIECES = 8
LANES = 128

NPA = 8


def apply_blocks(correlations, species_index, coupling, atom_start):
    rows = correlations.shape[0]
    count = correlations.shape[1] // NPA
    local_species = lax.dynamic_slice_in_dim(species_index, atom_start, count)
    onehot = (
        local_species[:, None] == jnp.arange(coupling.shape[0], dtype=jnp.int32)[None, :]
    ).astype(jnp.float32)
    blocks = jnp.einsum("as,sij->aij", onehot, coupling, precision=lax.Precision.HIGHEST)
    mixed = jnp.einsum(
        "baj,aij->bai",
        correlations.reshape(rows, count, NPA),
        blocks,
        precision=lax.Precision.HIGHEST,
    )
    return mixed.reshape(rows, count * NPA).astype(jnp.bfloat16)


def reduce_and_mix(partial_value, species_index, coupling, first_proj):
    total = lax.psum(partial_value.astype(jnp.bfloat16), "ga").astype(jnp.float32)
    return apply_blocks(total, species_index, coupling, first_proj // NPA)


def local(wavefunctions, projectors, kinetic_diag, species_index, coupling):
    proj_local = projectors.shape[0]
    band_index = lax.axis_index("band")
    partial_value = jnp.einsum(
        "bg,pg->bp",
        lax.all_gather(wavefunctions, "band", axis=0, tiled=True),
        projectors,
        preferred_element_type=jnp.float32,
    )
    mixed = reduce_and_mix(partial_value, species_index, coupling, band_index * proj_local)
    nonlocal_term = lax.psum_scatter(
        jnp.dot(mixed, projectors, preferred_element_type=jnp.float32).astype(jnp.bfloat16),
        "band",
        scatter_dimension=0,
        tiled=True,
    ).astype(jnp.float32)
    return (kinetic_diag[None, :] * wavefunctions.astype(jnp.float32) + nonlocal_term).astype(
        jnp.bfloat16
    )


EARLY = 2


def schedule():
    times = {
        "correlate": (0.3, 0.5, 16.6, 24.8),
        "forward": (None, None, 4.0, 9.5),
        "reduce": (7.5, 12.0, 29.7, 38.0),
        "join": (9.7, 15.0, 30.0, 39.5),
        "mix": (11.3, 16.3, 31.2, 40.7),
        "share": (14.4, 22.1, 36.1, 43.2),
        "expand": (22.2, 31.3, 43.5, 50.0),
        "settle": (57.0, None, None, None),
    }
    events = [
        (at, stage, k, 0)
        for stage, row in times.items()
        for k, at in enumerate(row)
        if at is not None
    ]
    for k, row in enumerate(((29.8, 29.82, 36.02, 36.04), (40.9, 40.92, 46.0, 46.1), (50.5, 51.5, 52.5, 53.5), (62.0, 63.0, 64.0, 65.0))):
        events += [(at, "far", k, t) for t, at in enumerate(row)]
    for k, first in enumerate((46.5, 52.6, 58.0, 70.0)):
        events += [(first + 0.05 * t, "near", k, t) for t in range(TILES)]
    return [event[1:] for event in sorted(events)]


def kernel(
    nga, wf, pj, kin_hbm, species_hbm, coupling_hbm, out,
    proj, wave, acc, csend, keep, parts, msend, mrecv, dsend, drecv, mixed,
    nsend, nrecv, own, nfull, ready, kin, species, coupling, tiles,
    s_send, s_loc, s_p, s_wm, s_wo, s_m, s_d, s_b, s_z, s_e, s_far, s_near, s_out, s_token,
):
    chunks, _, rows, half = wave.shape
    _, zn, share, both = csend.shape
    count = both // 2
    width = nsend.shape[-1]
    piece = half // PIECES
    quarter = zn // 4
    band, me = lax.axis_index("band"), lax.axis_index("ga")
    core, z, y, x = me % 2, me // 2, band // 2, band % 2
    across_x, across_y, diag = y * 2 + 1 - x, (1 - y) * 2 + x, 3 - band
    m = (1 - core) * y + core * x
    m_nbr = (1 - core) * across_y + core * across_x
    o_nbr = (1 - core) * across_x + core * across_y
    here = pl.multiple_of(m * half, LANES)
    there = pl.multiple_of((1 - m) * half, LANES)
    to_m, to_o, to_twin = {"band": m_nbr}, {"band": o_nbr}, {"ga": z * 2 + 1 - core}

    def remote(src, dst, sent, received, device):
        return pltpu.make_async_remote_copy(
            src_ref=src, dst_ref=dst, send_sem=s_send.at[sent], recv_sem=received,
            device_id=device, device_id_type=pl.DeviceIdType.MESH,
        )

    def span(k):
        return pl.ds(k * rows, rows)

    def peer(step):
        return (z + 1 + step) % zn

    def to_peer(step):
        return {"ga": peer(step) * 2 + core}

    local_p = pltpu.make_async_copy(pj.at[:, pl.ds(here, half)], proj.at[0], s_loc.at[0])
    local_k = pltpu.make_async_copy(kin_hbm.at[:, pl.ds(here, half)], kin, s_loc.at[1])
    local_s = pltpu.make_async_copy(species_hbm, species, s_loc.at[2])
    local_c = pltpu.make_async_copy(coupling_hbm, coupling, s_loc.at[4])
    local_w = [
        pltpu.make_async_copy(wf.at[span(k), pl.ds(here, half)], wave.at[k, band], s_loc.at[3])
        for k in range(chunks)
    ]
    send_p = [
        remote(
            pj.at[:, pl.ds(pl.multiple_of(there + i * piece, LANES), piece)],
            proj.at[1, :, pl.ds(i * piece, piece)], 0, s_p.at[i], to_m,
        )
        for i in range(PIECES)
    ]
    send_wm = [
        remote(wf.at[span(k), pl.ds(there, half)], wave.at[k, band], 1, s_wm.at[k], to_m)
        for k in range(chunks)
    ]
    send_wo = [
        remote(
            wf.at[span(k), pl.ds(here, half)], wave.at[k, band], 2,
            s_wo.at[max(k - EARLY + 1, 0)], to_o,
        )
        for k in range(chunks)
    ]
    send_wf = [
        remote(
            wave.at[k, m_nbr], wave.at[k, m_nbr], 3, s_wo.at[max(k - EARLY + 1, 0)], to_o
        )
        for k in range(chunks)
    ]
    send_m = [remote(msend.at[k], mrecv.at[k], 4, s_m.at[k], to_m) for k in range(chunks)]
    send_d = [remote(dsend.at[k], drecv.at[k], 5, s_d.at[k], to_twin) for k in range(chunks)]
    send_b = [
        remote(mixed.at[k, z, :, :count], mixed.at[k, z, :, count:], 6, s_b.at[k], to_m)
        for k in range(chunks)
    ]

    def send_z(k, step):
        return remote(csend.at[k, peer(step)], parts.at[k, step], 7, s_z.at[k], to_peer(step))

    def send_e(k, step):
        block = mixed.at[k, z, :, :count]
        return remote(block, block, 8, s_e.at[k], to_peer(step))

    def send_g(k, step):
        block = mixed.at[k, z, :, count:]
        return remote(block, block, 8, s_e.at[k], to_peer(step))

    def send_near(k):
        return remote(nsend.at[k, 0], nrecv.at[k, 0], 9, s_near.at[k], to_o)

    def send_n(k, t, side):
        received = s_far.at[k, t] if side else s_near.at[k + t]
        return remote(nsend.at[k, side, t], nrecv.at[k, side, t], 9, received, to_o)

    def place(k, t):
        return out.at[span(k), pl.ds(pl.multiple_of(here + t * width, LANES), width)]

    def send_o(k, t):
        return remote(nfull.at[k, t], place(k, t), 10, s_out.at[0], to_m)

    def write(k, t):
        return pltpu.make_async_copy(ready.at[k, t], place(k, t), s_out.at[1])

    def arrived(ref, semaphore):
        pltpu.make_async_copy(ref, ref, semaphore).wait()

    def each_peer(body):
        def step(i, carry):
            body(i)
            return carry

        lax.fori_loop(0, zn - 1, step, 0)

    def each_tile(body):
        def step(i, carry):
            body(i)
            return carry

        lax.fori_loop(0, TILES, step, 0)

    def columns(t):
        return pl.ds(pl.multiple_of(t * width, LANES), width)

    def add_product(chunk, slot, cols):
        product = lax.dot_general(
            wave[chunk, :, :, cols].reshape(-1, proj[slot, :, cols].shape[-1]),
            proj[slot, :, cols],
            (((1,), (1,)), ((), ())),
            preferred_element_type=jnp.float32,
        )
        product = product.reshape(-1, zn, share, count)
        acc[: product.shape[0], :, :, slot * count : (slot + 1) * count] += product

    def build_tiles():
        kinds, npa = coupling.shape[0], coupling.shape[1]
        atoms = species.shape[1]
        local_s.wait()
        local_c.wait()
        first = band * (count // npa)
        atom = lax.broadcasted_iota(jnp.int32, (atoms, count), 0)
        column = lax.broadcasted_iota(jnp.int32, (atoms, count), 1)
        spread = (atom == first + column // npa).astype(jnp.float32)
        kind = lax.broadcasted_iota(jnp.int32, (8, atoms), 0)
        onehot = (kind == species[...]).astype(jnp.float32)
        chosen = jnp.dot(
            onehot, spread, preferred_element_type=jnp.float32, precision=lax.Precision.HIGHEST
        )
        row = lax.broadcasted_iota(jnp.int32, (LANES, npa), 0)
        index = lax.broadcasted_iota(jnp.int32, (LANES, npa), 1)
        repeat = (row % npa == index).astype(jnp.float32)
        blocks = []
        for s in range(kinds):
            tall = lax.dot_general(
                repeat, coupling[s], (((1,), (1,)), ((), ())),
                preferred_element_type=jnp.float32, precision=lax.Precision.HIGHEST,
            )
            blocks.append(
                lax.dot_general(
                    tall, repeat, (((1,), (1,)), ((), ())),
                    preferred_element_type=jnp.float32, precision=lax.Precision.HIGHEST,
                )
            )
        atom_row = lax.broadcasted_iota(jnp.int32, (LANES, LANES), 0) // npa
        atom_col = lax.broadcasted_iota(jnp.int32, (LANES, LANES), 1) // npa
        same = atom_row == atom_col
        for t in range(tiles.shape[0]):
            value = jnp.zeros((LANES, LANES), jnp.float32)
            for s in range(kinds):
                here_kind = chosen[s : s + 1, t * LANES : (t + 1) * LANES]
                value = jnp.where(here_kind > 0.5, blocks[s], value)
            tiles[t] = jnp.where(same, value, 0.0)

    def forward(k):
        send_wm[k].wait_recv()
        if k == EARLY:
            send_wo[k].start()
        send_wf[k].start()
        if k == EARLY:
            for later in range(EARLY + 1, chunks):
                send_wo[later].start()

    def correlate(k):
        place = k
        if k >= EARLY:
            place = 0
            arrived(wave.at[k, pl.ds(0, 2)], s_wo.at[k - EARLY + 1])
            acc[0] = jnp.zeros_like(acc[0])

            def tile(t):
                add_product(slice(k, k + 1), 0, columns(t))
                add_product(slice(k, k + 1), 1, columns(t))

            each_tile(tile)
        csend[k] = acc[place].astype(jnp.bfloat16)
        each_peer(lambda step: send_z(k, step).start())
        keep[k] = acc[place, z]

    def reduce(k):
        arrived(parts.at[k], s_z.at[k])
        total = keep[k]
        for step in range(zn - 1):
            total = total + parts[k, step].astype(jnp.float32)
        msend[k] = total[:, count:].astype(jnp.bfloat16)
        send_m[k].start()
        dsend[k] = total[:, :count]

    def join(k):
        send_m[k].wait_recv()
        dsend[k] = dsend[k] + mrecv[k].astype(jnp.float32)
        send_d[k].start()

    def mix(k):
        send_d[k].wait_recv()
        total = dsend[k] + drecv[k]
        for t in range(tiles.shape[0]):
            cols = slice(t * LANES, (t + 1) * LANES)
            mixed[k, z, :, cols] = jnp.dot(
                total[:, cols], tiles[t],
                preferred_element_type=jnp.float32, precision=lax.Precision.HIGHEST,
            ).astype(jnp.bfloat16)
        send_b[k].start()
        each_peer(lambda step: send_e(k, step).start())

    def share_out(k):
        send_b[k].wait_recv()
        each_peer(lambda step: send_g(k, step).start())

    def expand(k):
        arrived(parts.at[k], s_e.at[k])

        def tile(t):
            cols = columns(t)
            picks = [
                mixed[k, pl.ds(b * quarter, quarter)].reshape(rows, both)
                for b in (o_nbr, diag, band, m_nbr)
            ]
            value = jnp.dot(
                jnp.concatenate(picks, axis=0), proj[:, :, cols].reshape(both, width),
                preferred_element_type=jnp.float32,
            ).reshape(4, rows, width)
            nsend[k, :, t] = value[:2].astype(jnp.bfloat16)
            send_n(k, t, 1).start()
            own[k, t] = value[2:]

        each_tile(tile)
        if k == chunks - 1:
            each_tile(lambda t: send_n(k, t, 0).start())
        else:
            send_near(k).start()

    def complete(k, t, side, owner):
        cols = columns(t)
        kinetic = kin[:, cols] * wave[k, owner, :, cols].astype(jnp.float32)
        total = own[k, t, side] + nrecv[k, side, t].astype(jnp.float32)
        return (kinetic + total).astype(jnp.bfloat16)

    def far(k, t):
        send_n(k, t, 1).wait_recv()
        nfull[k, t] = complete(k, t, 1, m_nbr)
        send_o(k, t).start()

    def near(k, t):
        if k == chunks - 1:
            send_n(k, t, 0).wait_recv()
        elif t == 0:
            send_near(k).wait_recv()
        ready[k, t] = complete(k, t, 0, band)
        write(k, t).start()

    barrier = pltpu.get_barrier_semaphore()

    def greet(semaphore, device):
        pl.semaphore_signal(
            semaphore, inc=1, device_id=device, device_id_type=pl.DeviceIdType.MESH
        )

    above, below = {"ga": (z + 1) * 2 + core}, {"ga": (z - 1) * 2 + core}
    has_above, has_below = z < zn - 1, z > 0
    for device in (to_m, to_o, to_twin):
        greet(barrier, device)
    pl.when(has_above)(lambda: greet(barrier, above))
    pl.when(has_below)(lambda: greet(barrier, below))
    local_p.start()
    for copy in local_w:
        copy.start()
    local_s.start()
    local_c.start()
    local_k.start()
    pl.semaphore_wait(barrier, 3 + has_above.astype(jnp.int32) + has_below.astype(jnp.int32))

    for k in range(EARLY):
        send_wm[k].start()
        send_wo[k].start()
    for copy in send_p:
        copy.start()
    for k in range(EARLY, chunks):
        send_wm[k].start()
    with jax.named_scope("tokens"):
        pl.when(has_below)(lambda: pl.semaphore_wait(s_token.at[0], 1))
        pl.when(has_above)(lambda: greet(s_token.at[0], above))
        pl.when(has_above)(lambda: pl.semaphore_wait(s_token.at[1], 1))
        pl.when(has_below)(lambda: greet(s_token.at[1], below))
    with jax.named_scope("build"):
        build_tiles()
    with jax.named_scope("first"):
        for k in range(EARLY):
            forward(k)
        local_k.wait()
        local_p.wait()
        arrived(wave.at[:, 0], s_loc.at[3])
        arrived(wave.at[pl.ds(0, EARLY), pl.ds(0, 2)], s_wo.at[0])
        acc[...] = jnp.zeros_like(acc)
        each_tile(lambda t: add_product(slice(0, EARLY), 0, columns(t)))
    for i in range(PIECES):
        with jax.named_scope(f"piece#i={i}"):
            send_p[i].wait_recv()
            add_product(slice(0, EARLY), 1, slice(i * piece, (i + 1) * piece))

    def settle(k):
        sent = (
            proj.at[1], wave.at[:, 0], wave.at[:, 0], wave.at[:, 0], mrecv, drecv, msend, parts, parts
        )
        for kind, ref in enumerate(sent):
            arrived(ref, s_send.at[kind])

    stages = {
        "forward": forward, "correlate": correlate, "reduce": reduce, "join": join, "mix": mix,
        "share": share_out, "expand": expand, "settle": settle,
    }
    for stage, k, t in schedule():
        with jax.named_scope(f"{stage}#k={k}#t={t}"):
            if stage == "far":
                far(k, t)
            elif stage == "near":
                near(k, t)
            else:
                stages[stage](k)
    with jax.named_scope("others"):
        arrived(ready, s_out.at[1])
        arrived(nsend, s_send.at[9])
        arrived(nfull, s_send.at[10])
    with jax.named_scope("last"):
        arrived(nfull, s_out.at[0])


def in_hbm(array):
    return pltpu.with_memory_space_constraint(array, pltpu.HBM)


def square(nga, wavefunctions, projectors, kinetic_diag, species_index, coupling):
    bands, waves = wavefunctions.shape
    count = projectors.shape[0]
    atoms = species_index.shape[0]
    half, rows = waves // 2, bands // CHUNKS
    zn = nga // 2
    width, share = half // TILES, 4 * rows // zn
    bf16, f32 = jnp.bfloat16, jnp.float32
    dma = pltpu.SemaphoreType.DMA
    anywhere = pl.BlockSpec(memory_space=pl.ANY)
    return pl.pallas_call(
        functools.partial(kernel, nga),
        out_shape=jax.ShapeDtypeStruct((bands, waves), bf16),
        in_specs=[anywhere] * 5,
        out_specs=anywhere,
        scratch_shapes=[
            pltpu.VMEM((2, count, half), bf16),
            pltpu.VMEM((CHUNKS, 4, rows, half), bf16),
            pltpu.VMEM((EARLY, zn, share, 2 * count), f32),
            pltpu.VMEM((CHUNKS, zn, share, 2 * count), bf16),
            pltpu.VMEM((CHUNKS, share, 2 * count), f32),
            pltpu.VMEM((CHUNKS, zn - 1, share, 2 * count), bf16),
            pltpu.VMEM((CHUNKS, share, count), bf16),
            pltpu.VMEM((CHUNKS, share, count), bf16),
            pltpu.VMEM((CHUNKS, share, count), f32),
            pltpu.VMEM((CHUNKS, share, count), f32),
            pltpu.VMEM((CHUNKS, zn, share, 2 * count), bf16),
            pltpu.VMEM((CHUNKS, 2, TILES, rows, width), bf16),
            pltpu.VMEM((CHUNKS, 2, TILES, rows, width), bf16),
            pltpu.VMEM((CHUNKS, TILES, 2, rows, width), f32),
            pltpu.VMEM((CHUNKS, TILES, rows, width), bf16),
            pltpu.VMEM((CHUNKS, TILES, rows, width), bf16),
            pltpu.VMEM((1, half), f32),
            pltpu.VMEM((1, atoms), jnp.int32),
            pltpu.VMEM(coupling.shape, f32),
            pltpu.VMEM((count // LANES, LANES, LANES), f32),
            dma((11,)),
            dma((5,)),
            dma((PIECES,)),
            dma((CHUNKS,)),
            dma((CHUNKS - EARLY + 1,)),
            dma((CHUNKS,)),
            dma((CHUNKS,)),
            dma((CHUNKS,)),
            dma((CHUNKS,)),
            dma((CHUNKS,)),
            dma((CHUNKS, TILES)),
            dma((CHUNKS + TILES - 1,)),
            dma((2,)),
            pltpu.SemaphoreType.REGULAR((2,)),
        ],
        compiler_params=pltpu.CompilerParams(
            collective_id=0, has_side_effects=True, vmem_limit_bytes=50 * 2**20
        ),
    )(
        wavefunctions, projectors, in_hbm(kinetic_diag.reshape(1, waves)),
        in_hbm(species_index.reshape(1, atoms)), in_hbm(coupling),
    )


def solution(mesh):
    in_specs = (P("band", "ga"), P("band", "ga"), P("ga"), P(), P())
    out_specs = P("band", "ga")
    nga = mesh.shape["ga"]
    fits = mesh.shape["band"] == 4 and nga % 8 == 0
    body = functools.partial(square, nga) if fits else local
    return jax.shard_map(body, mesh=mesh, in_specs=in_specs, out_specs=out_specs, check_vma=False)
```

```python
import functools

import jax
import jax.numpy as jnp
from jax import lax
from jax.experimental import pallas as pl
from jax.experimental.pallas import tpu as pltpu
from jax.sharding import PartitionSpec as P

CHUNKS = 4
TILES = 4
PIECES = 8
LANES = 128

NPA = 8


def apply_blocks(correlations, species_index, coupling, atom_start):
    rows = correlations.shape[0]
    count = correlations.shape[1] // NPA
    local_species = lax.dynamic_slice_in_dim(species_index, atom_start, count)
    onehot = (
        local_species[:, None] == jnp.arange(coupling.shape[0], dtype=jnp.int32)[None, :]
    ).astype(jnp.float32)
    blocks = jnp.einsum("as,sij->aij", onehot, coupling, precision=lax.Precision.HIGHEST)
    mixed = jnp.einsum(
        "baj,aij->bai",
        correlations.reshape(rows, count, NPA),
        blocks,
        precision=lax.Precision.HIGHEST,
    )
    return mixed.reshape(rows, count * NPA).astype(jnp.bfloat16)


def reduce_and_mix(partial_value, species_index, coupling, first_proj):
    total = lax.psum(partial_value.astype(jnp.bfloat16), "ga").astype(jnp.float32)
    return apply_blocks(total, species_index, coupling, first_proj // NPA)


def local(wavefunctions, projectors, kinetic_diag, species_index, coupling):
    proj_local = projectors.shape[0]
    band_index = lax.axis_index("band")
    partial_value = jnp.einsum(
        "bg,pg->bp",
        lax.all_gather(wavefunctions, "band", axis=0, tiled=True),
        projectors,
        preferred_element_type=jnp.float32,
    )
    mixed = reduce_and_mix(partial_value, species_index, coupling, band_index * proj_local)
    nonlocal_term = lax.psum_scatter(
        jnp.dot(mixed, projectors, preferred_element_type=jnp.float32).astype(jnp.bfloat16),
        "band",
        scatter_dimension=0,
        tiled=True,
    ).astype(jnp.float32)
    return (kinetic_diag[None, :] * wavefunctions.astype(jnp.float32) + nonlocal_term).astype(
        jnp.bfloat16
    )


EARLY = 2


def schedule():
    times = {
        "correlate": (0.3, 0.5, 16.6, 24.8),
        "forward": (None, None, 4.0, 9.5),
        "reduce": (7.5, 12.0, 29.7, 36.5),
        "join": (9.7, 15.0, 30.0, 38.0),
        "mix": (11.3, 16.3, 31.2, 39.2),
        "share": (14.4, 22.1, 36.1, 42.2),
        "expand": (22.2, 31.3, 42.0, 50.0),
        "turn": (1.0, None, None, None),
        "settle": (57.0, None, None, None),
    }
    events = [
        (at, stage, k, 0)
        for stage, row in times.items()
        for k, at in enumerate(row)
        if at is not None
    ]
    for k, row in enumerate(((29.8, 29.81, 29.82, 29.83), (39.6, 39.7, 39.8, 39.9), (50.5, 51.5, 52.5, 53.5), (62.0, 63.0, 64.0, 65.0))):
        events += [(at, "far", k, t) for t, at in enumerate(row)]
    for k, first in enumerate((46.5, 52.6, 58.0, 70.0)):
        events += [(first + 0.05 * t, "near", k, t) for t in range(TILES)]
    return [event[1:] for event in sorted(events)]


def kernel(
    nga, wf, pj, kin_hbm, species_hbm, coupling_hbm, out,
    proj, flip, wave, acc, csend, keep, parts, msend, mrecv, dsend, drecv, mixed,
    nsend, nrecv, own, nfull, kin, species, coupling, tiles,
    s_send, s_loc, s_p, s_wm, s_wo, s_m, s_d, s_b, s_z, s_e, s_far, s_near, s_out, s_token,
):
    chunks, _, rows, half = wave.shape
    _, zn, share, both = csend.shape
    count = both // 2
    width = nsend.shape[-1]
    piece = half // PIECES
    quarter = zn // 4
    band, me = lax.axis_index("band"), lax.axis_index("ga")
    core, z, y, x = me % 2, me // 2, band // 2, band % 2
    across_x, across_y, diag = y * 2 + 1 - x, (1 - y) * 2 + x, 3 - band
    m = (1 - core) * y + core * x
    m_nbr = (1 - core) * across_y + core * across_x
    o_nbr = (1 - core) * across_x + core * across_y
    here = pl.multiple_of(m * half, LANES)
    there = pl.multiple_of((1 - m) * half, LANES)
    to_m, to_o, to_twin = {"band": m_nbr}, {"band": o_nbr}, {"ga": z * 2 + 1 - core}

    def remote(src, dst, sent, received, device):
        return pltpu.make_async_remote_copy(
            src_ref=src, dst_ref=dst, send_sem=s_send.at[sent], recv_sem=received,
            device_id=device, device_id_type=pl.DeviceIdType.MESH,
        )

    def span(k):
        return pl.ds(k * rows, rows)

    def peer(step):
        return (z + 1 + step) % zn

    def to_peer(step):
        return {"ga": peer(step) * 2 + core}

    local_p = pltpu.make_async_copy(pj.at[:, pl.ds(here, half)], proj.at[0], s_loc.at[0])
    local_k = pltpu.make_async_copy(kin_hbm.at[:, pl.ds(here, half)], kin, s_loc.at[1])
    local_s = pltpu.make_async_copy(species_hbm, species, s_loc.at[2])
    local_c = pltpu.make_async_copy(coupling_hbm, coupling, s_loc.at[4])
    local_w = [
        pltpu.make_async_copy(wf.at[span(k), pl.ds(here, half)], wave.at[k, band], s_loc.at[3])
        for k in range(chunks)
    ]
    send_p = [
        remote(
            pj.at[:, pl.ds(pl.multiple_of(there + i * piece, LANES), piece)],
            proj.at[1, :, pl.ds(i * piece, piece)], 0, s_p.at[i], to_m,
        )
        for i in range(PIECES)
    ]
    send_wm = [
        remote(wf.at[span(k), pl.ds(there, half)], wave.at[k, band], 1, s_wm.at[k], to_m)
        for k in range(chunks)
    ]
    send_wo = [
        remote(
            wf.at[span(k), pl.ds(here, half)], wave.at[k, band], 2,
            s_wo.at[max(k - EARLY + 1, 0)], to_o,
        )
        for k in range(chunks)
    ]
    send_wf = [
        remote(
            wave.at[k, m_nbr], wave.at[k, m_nbr], 3, s_wo.at[max(k - EARLY + 1, 0)], to_o
        )
        for k in range(chunks)
    ]
    send_m = [remote(msend.at[k], mrecv.at[k], 4, s_m.at[k], to_m) for k in range(chunks)]
    send_d = [remote(dsend.at[k], drecv.at[k], 5, s_d.at[k], to_twin) for k in range(chunks)]
    send_b = [
        remote(mixed.at[k, z, :, :count], mixed.at[k, z, :, count:], 6, s_b.at[k], to_m)
        for k in range(chunks)
    ]

    def send_z(k, step):
        return remote(csend.at[k, peer(step)], parts.at[k, step], 7, s_z.at[k], to_peer(step))

    def send_e(k, step):
        block = mixed.at[k, z, :, :count]
        return remote(block, block, 8, s_e.at[k], to_peer(step))

    def send_g(k, step):
        block = mixed.at[k, z, :, count:]
        return remote(block, block, 8, s_e.at[k], to_peer(step))

    def send_near(k):
        return remote(nsend.at[k, 0], nrecv.at[k, 0], 9, s_near.at[k], to_o)

    def send_n(k, t, side):
        received = s_far.at[k, t] if side else s_near.at[k + t]
        return remote(nsend.at[k, side, t], nrecv.at[k, side, t], 9, received, to_o)

    def place(k, t):
        return out.at[span(k), pl.ds(pl.multiple_of(here + t * width, LANES), width)]

    def send_o(k, t):
        return remote(nfull.at[k, t], place(k, t), 10, s_out.at[0], to_m)

    def arrived(ref, semaphore):
        pltpu.make_async_copy(ref, ref, semaphore).wait()

    def each_peer(body):
        def step(i, carry):
            body(i)
            return carry

        lax.fori_loop(0, zn - 1, step, 0)

    def each_tile(body):
        def step(i, carry):
            body(i)
            return carry

        lax.fori_loop(0, TILES, step, 0)

    def columns(t):
        return pl.ds(pl.multiple_of(t * width, LANES), width)

    def add_product(chunk, slot, cols):
        product = lax.dot_general(
            wave[chunk, :, :, cols].reshape(-1, proj[slot, :, cols].shape[-1]),
            proj[slot, :, cols],
            (((1,), (1,)), ((), ())),
            preferred_element_type=jnp.float32,
        )
        product = product.reshape(-1, zn, share, count)
        acc[: product.shape[0], :, :, slot * count : (slot + 1) * count] += product

    def turn(slot, i):
        part = pl.ds(pl.multiple_of(i * piece, LANES), piece)
        flip[part, slot * count : (slot + 1) * count] = proj[slot, :, part].T

    def turn_own(i, carry):
        turn(0, i)
        return carry

    def build_tiles():
        kinds, npa = coupling.shape[0], coupling.shape[1]
        atoms = species.shape[1]
        local_s.wait()
        local_c.wait()
        first = band * (count // npa)
        atom = lax.broadcasted_iota(jnp.int32, (atoms, count), 0)
        column = lax.broadcasted_iota(jnp.int32, (atoms, count), 1)
        spread = (atom == first + column // npa).astype(jnp.float32)
        kind = lax.broadcasted_iota(jnp.int32, (8, atoms), 0)
        onehot = (kind == species[...]).astype(jnp.float32)
        chosen = jnp.dot(
            onehot, spread, preferred_element_type=jnp.float32, precision=lax.Precision.HIGHEST
        )
        row = lax.broadcasted_iota(jnp.int32, (LANES, npa), 0)
        index = lax.broadcasted_iota(jnp.int32, (LANES, npa), 1)
        repeat = (row % npa == index).astype(jnp.float32)
        blocks = []
        for s in range(kinds):
            tall = lax.dot_general(
                repeat, coupling[s], (((1,), (1,)), ((), ())),
                preferred_element_type=jnp.float32, precision=lax.Precision.HIGHEST,
            )
            blocks.append(
                lax.dot_general(
                    tall, repeat, (((1,), (1,)), ((), ())),
                    preferred_element_type=jnp.float32, precision=lax.Precision.HIGHEST,
                )
            )
        atom_row = lax.broadcasted_iota(jnp.int32, (LANES, LANES), 0) // npa
        atom_col = lax.broadcasted_iota(jnp.int32, (LANES, LANES), 1) // npa
        same = atom_row == atom_col
        for t in range(tiles.shape[0]):
            value = jnp.zeros((LANES, LANES), jnp.float32)
            for s in range(kinds):
                here_kind = chosen[s : s + 1, t * LANES : (t + 1) * LANES]
                value = jnp.where(here_kind > 0.5, blocks[s], value)
            tiles[t] = jnp.where(same, value, 0.0)

    def forward(k):
        send_wm[k].wait_recv()
        if k == EARLY:
            send_wo[k].start()
        send_wf[k].start()
        if k == EARLY:
            for later in range(EARLY + 1, chunks):
                send_wo[later].start()

    def correlate(k):
        place = k
        if k >= EARLY:
            place = 0
            arrived(wave.at[k, pl.ds(0, 2)], s_wo.at[k - EARLY + 1])
            acc[0] = jnp.zeros_like(acc[0])

            def tile(t):
                product = jnp.dot(
                    wave[k, :, :, columns(t)].reshape(4 * rows, width), flip[columns(t), :],
                    preferred_element_type=jnp.float32,
                )
                acc[0] += product.reshape(zn, share, both)

            each_tile(tile)
        csend[k] = acc[place].astype(jnp.bfloat16)
        each_peer(lambda step: send_z(k, step).start())
        keep[k] = acc[place, z]

    def reduce(k):
        arrived(parts.at[k], s_z.at[k])
        total = keep[k]
        for step in range(zn - 1):
            total = total + parts[k, step].astype(jnp.float32)
        msend[k] = total[:, count:].astype(jnp.bfloat16)
        send_m[k].start()
        dsend[k] = total[:, :count]

    def join(k):
        send_m[k].wait_recv()
        dsend[k] = dsend[k] + mrecv[k].astype(jnp.float32)
        send_d[k].start()

    def mix(k):
        send_d[k].wait_recv()
        total = dsend[k] + drecv[k]
        for t in range(tiles.shape[0]):
            cols = slice(t * LANES, (t + 1) * LANES)
            mixed[k, z, :, cols] = jnp.dot(
                total[:, cols], tiles[t],
                preferred_element_type=jnp.float32, precision=lax.Precision.HIGHEST,
            ).astype(jnp.bfloat16)
        send_b[k].start()
        each_peer(lambda step: send_e(k, step).start())

    def share_out(k):
        send_b[k].wait_recv()
        each_peer(lambda step: send_g(k, step).start())

    def expand(k):
        arrived(parts.at[k], s_e.at[k])

        def tile(t):
            cols = columns(t)
            picks = [
                mixed[k, pl.ds(b * quarter, quarter)].reshape(rows, both)
                for b in (o_nbr, diag, band, m_nbr)
            ]
            value = jnp.dot(
                jnp.concatenate(picks, axis=0), proj[:, :, cols].reshape(both, width),
                preferred_element_type=jnp.float32,
            ).reshape(4, rows, width)
            nsend[k, :, t] = value[:2].astype(jnp.bfloat16)
            send_n(k, t, 1).start()
            own[k % 3, t] = value[2:]

        each_tile(tile)
        if k == chunks - 1:
            each_tile(lambda t: send_n(k, t, 0).start())
        else:
            send_near(k).start()

    def complete(k, t, side, owner):
        cols = columns(t)
        kinetic = kin[:, cols] * wave[k, owner, :, cols].astype(jnp.float32)
        total = own[k % 3, t, side] + nrecv[k, side, t].astype(jnp.float32)
        return (kinetic + total).astype(jnp.bfloat16)

    def far(k, t):
        send_n(k, t, 1).wait_recv()
        nfull[k, t] = complete(k, t, 1, m_nbr)
        send_o(k, t).start()

    def near(k, t):
        if k == chunks - 1:
            send_n(k, t, 0).wait_recv()
        elif t == 0:
            send_near(k).wait_recv()
        out[span(k), pl.ds(pl.multiple_of(here + t * width, LANES), width)] = complete(
            k, t, 0, band
        )

    barrier = pltpu.get_barrier_semaphore()

    def greet(semaphore, device):
        pl.semaphore_signal(
            semaphore, inc=1, device_id=device, device_id_type=pl.DeviceIdType.MESH
        )

    above, below = {"ga": (z + 1) * 2 + core}, {"ga": (z - 1) * 2 + core}
    has_above, has_below = z < zn - 1, z > 0
    for device in (to_m, to_o, to_twin):
        greet(barrier, device)
    pl.when(has_above)(lambda: greet(barrier, above))
    pl.when(has_below)(lambda: greet(barrier, below))
    local_p.start()
    for copy in local_w:
        copy.start()
    local_s.start()
    local_c.start()
    local_k.start()
    pl.semaphore_wait(barrier, 3 + has_above.astype(jnp.int32) + has_below.astype(jnp.int32))

    for k in range(EARLY):
        send_wm[k].start()
        send_wo[k].start()
    for copy in send_p:
        copy.start()
    for k in range(EARLY, chunks):
        send_wm[k].start()
    with jax.named_scope("tokens"):
        pl.when(has_below)(lambda: pl.semaphore_wait(s_token.at[0], 1))
        pl.when(has_above)(lambda: greet(s_token.at[0], above))
        pl.when(has_above)(lambda: pl.semaphore_wait(s_token.at[1], 1))
        pl.when(has_below)(lambda: greet(s_token.at[1], below))
    with jax.named_scope("build"):
        build_tiles()
    with jax.named_scope("first"):
        for k in range(EARLY):
            forward(k)
        local_k.wait()
        local_p.wait()
        arrived(wave.at[:, 0], s_loc.at[3])
        arrived(wave.at[pl.ds(0, EARLY), pl.ds(0, 2)], s_wo.at[0])
        acc[...] = jnp.zeros_like(acc)
        each_tile(lambda t: add_product(slice(0, EARLY), 0, columns(t)))
        lax.fori_loop(0, PIECES, turn_own, 0)
    for i in range(PIECES):
        with jax.named_scope(f"piece#i={i}"):
            send_p[i].wait_recv()
            add_product(slice(0, EARLY), 1, slice(i * piece, (i + 1) * piece))
            if i < PIECES - 1:
                turn(1, i)

    def settle(k):
        sent = (
            proj.at[1], wave.at[:, 0], wave.at[:, 0], wave.at[:, 0], mrecv, drecv, msend, parts, parts
        )
        for kind, ref in enumerate(sent):
            arrived(ref, s_send.at[kind])

    stages = {
        "forward": forward, "correlate": correlate, "reduce": reduce, "join": join, "mix": mix,
        "share": share_out, "expand": expand, "settle": settle,
    }
    def turn_last(k):
        turn(1, PIECES - 1)

    stages["turn"] = turn_last
    for stage, k, t in schedule():
        with jax.named_scope(f"{stage}#k={k}#t={t}"):
            if stage == "far":
                far(k, t)
            elif stage == "near":
                near(k, t)
            else:
                stages[stage](k)
    with jax.named_scope("others"):
        arrived(nsend, s_send.at[9])
        arrived(nfull, s_send.at[10])
    with jax.named_scope("last"):
        arrived(nfull, s_out.at[0])


def in_hbm(array):
    return pltpu.with_memory_space_constraint(array, pltpu.HBM)


def square(nga, wavefunctions, projectors, kinetic_diag, species_index, coupling):
    bands, waves = wavefunctions.shape
    count = projectors.shape[0]
    atoms = species_index.shape[0]
    half, rows = waves // 2, bands // CHUNKS
    zn = nga // 2
    width, share = half // TILES, 4 * rows // zn
    bf16, f32 = jnp.bfloat16, jnp.float32
    dma = pltpu.SemaphoreType.DMA
    anywhere = pl.BlockSpec(memory_space=pl.ANY)
    return pl.pallas_call(
        functools.partial(kernel, nga),
        out_shape=jax.ShapeDtypeStruct((bands, waves), bf16),
        in_specs=[anywhere] * 5,
        out_specs=pl.BlockSpec(memory_space=pltpu.VMEM),
        scratch_shapes=[
            pltpu.VMEM((2, count, half), bf16),
            pltpu.VMEM((half, 2 * count), bf16),
            pltpu.VMEM((CHUNKS, 4, rows, half), bf16),
            pltpu.VMEM((EARLY, zn, share, 2 * count), f32),
            pltpu.VMEM((CHUNKS, zn, share, 2 * count), bf16),
            pltpu.VMEM((CHUNKS, share, 2 * count), f32),
            pltpu.VMEM((CHUNKS, zn - 1, share, 2 * count), bf16),
            pltpu.VMEM((CHUNKS, share, count), bf16),
            pltpu.VMEM((CHUNKS, share, count), bf16),
            pltpu.VMEM((CHUNKS, share, count), f32),
            pltpu.VMEM((CHUNKS, share, count), f32),
            pltpu.VMEM((CHUNKS, zn, share, 2 * count), bf16),
            pltpu.VMEM((CHUNKS, 2, TILES, rows, width), bf16),
            pltpu.VMEM((CHUNKS, 2, TILES, rows, width), bf16),
            pltpu.VMEM((3, TILES, 2, rows, width), f32),
            pltpu.VMEM((CHUNKS, TILES, rows, width), bf16),
            pltpu.VMEM((1, half), f32),
            pltpu.VMEM((1, atoms), jnp.int32),
            pltpu.VMEM(coupling.shape, f32),
            pltpu.VMEM((count // LANES, LANES, LANES), f32),
            dma((11,)),
            dma((5,)),
            dma((PIECES,)),
            dma((CHUNKS,)),
            dma((CHUNKS - EARLY + 1,)),
            dma((CHUNKS,)),
            dma((CHUNKS,)),
            dma((CHUNKS,)),
            dma((CHUNKS,)),
            dma((CHUNKS,)),
            dma((CHUNKS, TILES)),
            dma((CHUNKS + TILES - 1,)),
            dma((1,)),
            pltpu.SemaphoreType.REGULAR((2,)),
        ],
        compiler_params=pltpu.CompilerParams(
            collective_id=0, has_side_effects=True, vmem_limit_bytes=53_300_000
        ),
    )(
        wavefunctions, projectors, in_hbm(kinetic_diag.reshape(1, waves)),
        in_hbm(species_index.reshape(1, atoms)), in_hbm(coupling),
    )


def solution(mesh):
    in_specs = (P("band", "ga"), P("band", "ga"), P("ga"), P(), P())
    out_specs = P("band", "ga")
    nga = mesh.shape["ga"]
    fits = mesh.shape["band"] == 4 and nga % 8 == 0
    body = functools.partial(square, nga) if fits else local
    return jax.shard_map(body, mesh=mesh, in_specs=in_specs, out_specs=out_specs, check_vma=False)
```

```python
import functools

import jax
import jax.numpy as jnp
from jax import lax
from jax.experimental import pallas as pl
from jax.experimental.pallas import tpu as pltpu
from jax.sharding import PartitionSpec as P

CHUNKS = 4
TILES = 4
PIECES = 8
LANES = 128

NPA = 8


def apply_blocks(correlations, species_index, coupling, atom_start):
    rows = correlations.shape[0]
    count = correlations.shape[1] // NPA
    local_species = lax.dynamic_slice_in_dim(species_index, atom_start, count)
    onehot = (
        local_species[:, None] == jnp.arange(coupling.shape[0], dtype=jnp.int32)[None, :]
    ).astype(jnp.float32)
    blocks = jnp.einsum("as,sij->aij", onehot, coupling, precision=lax.Precision.HIGHEST)
    mixed = jnp.einsum(
        "baj,aij->bai",
        correlations.reshape(rows, count, NPA),
        blocks,
        precision=lax.Precision.HIGHEST,
    )
    return mixed.reshape(rows, count * NPA).astype(jnp.bfloat16)


def reduce_and_mix(partial_value, species_index, coupling, first_proj):
    total = lax.psum(partial_value.astype(jnp.bfloat16), "ga").astype(jnp.float32)
    return apply_blocks(total, species_index, coupling, first_proj // NPA)


def local(wavefunctions, projectors, kinetic_diag, species_index, coupling):
    proj_local = projectors.shape[0]
    band_index = lax.axis_index("band")
    partial_value = jnp.einsum(
        "bg,pg->bp",
        lax.all_gather(wavefunctions, "band", axis=0, tiled=True),
        projectors,
        preferred_element_type=jnp.float32,
    )
    mixed = reduce_and_mix(partial_value, species_index, coupling, band_index * proj_local)
    nonlocal_term = lax.psum_scatter(
        jnp.dot(mixed, projectors, preferred_element_type=jnp.float32).astype(jnp.bfloat16),
        "band",
        scatter_dimension=0,
        tiled=True,
    ).astype(jnp.float32)
    return (kinetic_diag[None, :] * wavefunctions.astype(jnp.float32) + nonlocal_term).astype(
        jnp.bfloat16
    )


EARLY = 2


def schedule():
    times = {
        "correlate": (0.3, 0.5, 16.6, 24.8),
        "forward": (None, None, 4.0, 9.5),
        "reduce": (7.5, 12.0, 29.7, 36.5),
        "join": (9.7, 15.0, 30.0, 38.0),
        "mix": (11.3, 16.3, 31.2, 39.2),
        "share": (14.4, 22.1, 36.1, 42.2),
        "expand": (22.2, 31.3, 42.0, 50.0),
        "turn": (1.0, None, None, None),
        "settle": (57.0, None, None, None),
    }
    events = [
        (at, stage, k, 0)
        for stage, row in times.items()
        for k, at in enumerate(row)
        if at is not None
    ]
    for k, row in enumerate(((29.8, 29.81, 29.82, 29.83), (39.6, 39.7, 39.8, 39.9), (50.5, 51.5, 52.5, 53.5), (62.0, 63.0, 64.0, 65.0))):
        events += [(at, "far", k, t) for t, at in enumerate(row)]
    for k, first in enumerate((46.5, 52.6, 58.0, 70.0)):
        events += [(first + 0.05 * t, "near", k, t) for t in range(TILES)]
    return [event[1:] for event in sorted(events)]


def kernel(
    nga, wf, pj, kin_hbm, species_hbm, coupling_hbm, out,
    proj, flip, wave, acc, csend, keep, parts, msend, mrecv, dsend, drecv, mixed,
    nsend, nrecv, own, nfull, kin, species, coupling, tiles,
    s_send, s_loc, s_p, s_wm, s_wo, s_m, s_d, s_b, s_z, s_e, s_far, s_near, s_out, s_token,
):
    chunks, _, rows, half = wave.shape
    _, zn, share, both = csend.shape
    count = both // 2
    width = nsend.shape[-1]
    piece = half // PIECES
    quarter = zn // 4
    band, me = lax.axis_index("band"), lax.axis_index("ga")
    core, z, y, x = me % 2, me // 2, band // 2, band % 2
    across_x, across_y, diag = y * 2 + 1 - x, (1 - y) * 2 + x, 3 - band
    m = (1 - core) * y + core * x
    m_nbr = (1 - core) * across_y + core * across_x
    o_nbr = (1 - core) * across_x + core * across_y
    here = pl.multiple_of(m * half, LANES)
    there = pl.multiple_of((1 - m) * half, LANES)
    to_m, to_o, to_twin = {"band": m_nbr}, {"band": o_nbr}, {"ga": z * 2 + 1 - core}

    def remote(src, dst, sent, received, device):
        return pltpu.make_async_remote_copy(
            src_ref=src, dst_ref=dst, send_sem=s_send.at[sent], recv_sem=received,
            device_id=device, device_id_type=pl.DeviceIdType.MESH,
        )

    def span(k):
        return pl.ds(k * rows, rows)

    def peer(step):
        return (z + 1 + step) % zn

    def to_peer(step):
        return {"ga": peer(step) * 2 + core}

    local_p = pltpu.make_async_copy(pj.at[:, pl.ds(here, half)], proj.at[0], s_loc.at[0])
    local_k = pltpu.make_async_copy(kin_hbm.at[:, pl.ds(here, half)], kin, s_loc.at[1])
    local_s = pltpu.make_async_copy(species_hbm, species, s_loc.at[2])
    local_c = pltpu.make_async_copy(coupling_hbm, coupling, s_loc.at[4])
    local_w = [
        pltpu.make_async_copy(wf.at[span(k), pl.ds(here, half)], wave.at[k, band], s_loc.at[3])
        for k in range(chunks)
    ]
    send_p = [
        remote(
            pj.at[:, pl.ds(pl.multiple_of(there + i * piece, LANES), piece)],
            proj.at[1, :, pl.ds(i * piece, piece)], 0, s_p.at[i], to_m,
        )
        for i in range(PIECES)
    ]
    send_wm = [
        remote(wf.at[span(k), pl.ds(there, half)], wave.at[k, band], 1, s_wm.at[k], to_m)
        for k in range(chunks)
    ]
    send_wo = [
        remote(
            wf.at[span(k), pl.ds(here, half)], wave.at[k, band], 1,
            s_wo.at[max(k - EARLY + 1, 0)], to_o,
        )
        for k in range(chunks)
    ]
    send_wf = [
        remote(
            wave.at[k, m_nbr], wave.at[k, m_nbr], 1, s_wo.at[max(k - EARLY + 1, 0)], to_o
        )
        for k in range(chunks)
    ]
    send_m = [remote(msend.at[k], mrecv.at[k], 4, s_m.at[k], to_m) for k in range(chunks)]
    send_d = [remote(dsend.at[k], drecv.at[k], 2, s_d.at[k], to_twin) for k in range(chunks)]
    send_b = [
        remote(mixed.at[k, z, :, :count], mixed.at[k, z, :, count:], 4, s_b.at[k], to_m)
        for k in range(chunks)
    ]

    def send_z(k, step):
        return remote(csend.at[k, peer(step)], parts.at[k, step], 3, s_z.at[k], to_peer(step))

    def send_e(k, step):
        block = mixed.at[k, z, :, :count]
        return remote(block, block, 5, s_e.at[k], to_peer(step))

    def send_g(k, step):
        block = mixed.at[k, z, :, count:]
        return remote(block, block, 5, s_e.at[k], to_peer(step))

    def send_near(k):
        return remote(nsend.at[k, 0], nrecv.at[k, 0], 6, s_near.at[k], to_o)

    def send_n(k, t, side):
        received = s_far.at[k if k < 2 else 2 + (k - 2) * TILES + t] if side else s_near.at[k + t]
        return remote(nsend.at[k, side, t], nrecv.at[k, side, t], 6, received, to_o)

    def place(k, t):
        return out.at[span(k), pl.ds(pl.multiple_of(here + t * width, LANES), width)]

    def send_o(k, t):
        return remote(nfull.at[k, t], place(k, t), 7, s_out.at[0], to_m)

    def arrived(ref, semaphore):
        pltpu.make_async_copy(ref, ref, semaphore).wait()

    def each_peer(body):
        def step(i, carry):
            body(i)
            return carry

        lax.fori_loop(0, zn - 1, step, 0)

    def each_tile(body):
        def step(i, carry):
            body(i)
            return carry

        lax.fori_loop(0, TILES, step, 0)

    def columns(t):
        return pl.ds(pl.multiple_of(t * width, LANES), width)

    def add_product(chunk, slot, cols):
        product = lax.dot_general(
            wave[chunk, :, :, cols].reshape(-1, proj[slot, :, cols].shape[-1]),
            proj[slot, :, cols],
            (((1,), (1,)), ((), ())),
            preferred_element_type=jnp.float32,
        )
        product = product.reshape(-1, zn, share, count)
        acc[: product.shape[0], :, :, slot * count : (slot + 1) * count] += product

    def turn(slot, i):
        part = pl.ds(pl.multiple_of(i * piece, LANES), piece)
        flip[part, slot * count : (slot + 1) * count] = proj[slot, :, part].T

    def turn_own(i, carry):
        turn(0, i)
        return carry

    def build_tiles():
        kinds, npa = coupling.shape[0], coupling.shape[1]
        atoms = species.shape[1]
        local_s.wait()
        local_c.wait()
        first = band * (count // npa)
        atom = lax.broadcasted_iota(jnp.int32, (atoms, count), 0)
        column = lax.broadcasted_iota(jnp.int32, (atoms, count), 1)
        spread = (atom == first + column // npa).astype(jnp.float32)
        kind = lax.broadcasted_iota(jnp.int32, (8, atoms), 0)
        onehot = (kind == species[...]).astype(jnp.float32)
        chosen = jnp.dot(
            onehot, spread, preferred_element_type=jnp.float32, precision=lax.Precision.HIGHEST
        )
        row = lax.broadcasted_iota(jnp.int32, (LANES, npa), 0)
        index = lax.broadcasted_iota(jnp.int32, (LANES, npa), 1)
        repeat = (row % npa == index).astype(jnp.float32)
        blocks = []
        for s in range(kinds):
            tall = lax.dot_general(
                repeat, coupling[s], (((1,), (1,)), ((), ())),
                preferred_element_type=jnp.float32, precision=lax.Precision.HIGHEST,
            )
            blocks.append(
                lax.dot_general(
                    tall, repeat, (((1,), (1,)), ((), ())),
                    preferred_element_type=jnp.float32, precision=lax.Precision.HIGHEST,
                )
            )
        atom_row = lax.broadcasted_iota(jnp.int32, (LANES, LANES), 0) // npa
        atom_col = lax.broadcasted_iota(jnp.int32, (LANES, LANES), 1) // npa
        same = atom_row == atom_col
        for t in range(tiles.shape[0]):
            value = jnp.zeros((LANES, LANES), jnp.float32)
            for s in range(kinds):
                here_kind = chosen[s : s + 1, t * LANES : (t + 1) * LANES]
                value = jnp.where(here_kind > 0.5, blocks[s], value)
            tiles[t] = jnp.where(same, value, 0.0)

    def forward(k):
        send_wm[k].wait_recv()
        if k == EARLY:
            send_wo[k].start()
        send_wf[k].start()
        if k == EARLY:
            for later in range(EARLY + 1, chunks):
                send_wo[later].start()

    def correlate(k):
        place = k
        if k >= EARLY:
            place = 0
            arrived(wave.at[k, pl.ds(0, 2)], s_wo.at[k - EARLY + 1])
            acc[0] = jnp.zeros_like(acc[0])

            def tile(t):
                product = jnp.dot(
                    wave[k, :, :, columns(t)].reshape(4 * rows, width), flip[columns(t), :],
                    preferred_element_type=jnp.float32,
                )
                acc[0] += product.reshape(zn, share, both)

            each_tile(tile)
        csend[k] = acc[place].astype(jnp.bfloat16)
        each_peer(lambda step: send_z(k, step).start())
        keep[k] = acc[place, z]

    def reduce(k):
        arrived(parts.at[k], s_z.at[k])
        total = keep[k]
        for step in range(zn - 1):
            total = total + parts[k, step].astype(jnp.float32)
        msend[k] = total[:, count:].astype(jnp.bfloat16)
        send_m[k].start()
        dsend[k] = total[:, :count]

    def join(k):
        send_m[k].wait_recv()
        dsend[k] = dsend[k] + mrecv[k].astype(jnp.float32)
        send_d[k].start()

    def mix(k):
        send_d[k].wait_recv()
        total = dsend[k] + drecv[k]
        for t in range(tiles.shape[0]):
            cols = slice(t * LANES, (t + 1) * LANES)
            mixed[k, z, :, cols] = jnp.dot(
                total[:, cols], tiles[t],
                preferred_element_type=jnp.float32, precision=lax.Precision.HIGHEST,
            ).astype(jnp.bfloat16)
        send_b[k].start()
        each_peer(lambda step: send_e(k, step).start())

    def share_out(k):
        send_b[k].wait_recv()
        each_peer(lambda step: send_g(k, step).start())

    def expand(k):
        arrived(parts.at[k], s_e.at[k])

        def tile(t):
            cols = columns(t)
            picks = [
                mixed[k, pl.ds(b * quarter, quarter)].reshape(rows, both)
                for b in (o_nbr, diag, band, m_nbr)
            ]
            value = jnp.dot(
                jnp.concatenate(picks, axis=0), proj[:, :, cols].reshape(both, width),
                preferred_element_type=jnp.float32,
            ).reshape(4, rows, width)
            nsend[k, :, t] = value[:2].astype(jnp.bfloat16)
            send_n(k, t, 1).start()
            own[k % 3, t] = value[2:]

        each_tile(tile)
        if k == chunks - 1:
            each_tile(lambda t: send_n(k, t, 0).start())
        else:
            send_near(k).start()

    def complete(k, t, side, owner):
        cols = columns(t)
        kinetic = kin[:, cols] * wave[k, owner, :, cols].astype(jnp.float32)
        total = own[k % 3, t, side] + nrecv[k, side, t].astype(jnp.float32)
        return (kinetic + total).astype(jnp.bfloat16)

    def far(k, t):
        if k >= 2:
            send_n(k, t, 1).wait_recv()
        elif t == 0:
            arrived(nrecv.at[k, 1], s_far.at[k])
        nfull[k, t] = complete(k, t, 1, m_nbr)
        send_o(k, t).start()

    def near(k, t):
        if k == chunks - 1:
            send_n(k, t, 0).wait_recv()
        elif t == 0:
            send_near(k).wait_recv()
        out[span(k), pl.ds(pl.multiple_of(here + t * width, LANES), width)] = complete(
            k, t, 0, band
        )

    barrier = pltpu.get_barrier_semaphore()

    def greet(semaphore, device):
        pl.semaphore_signal(
            semaphore, inc=1, device_id=device, device_id_type=pl.DeviceIdType.MESH
        )

    above, below = {"ga": (z + 1) * 2 + core}, {"ga": (z - 1) * 2 + core}
    has_above, has_below = z < zn - 1, z > 0
    for device in (to_m, to_o, to_twin):
        greet(barrier, device)
    pl.when(has_above)(lambda: greet(barrier, above))
    pl.when(has_below)(lambda: greet(barrier, below))
    local_p.start()
    for copy in local_w:
        copy.start()
    local_s.start()
    local_c.start()
    local_k.start()
    pl.semaphore_wait(barrier, 3 + has_above.astype(jnp.int32) + has_below.astype(jnp.int32))

    for k in range(EARLY):
        send_wm[k].start()
        send_wo[k].start()
    for copy in send_p:
        copy.start()
    for k in range(EARLY, chunks):
        send_wm[k].start()
    with jax.named_scope("tokens"):
        pl.when(has_below)(lambda: pl.semaphore_wait(s_token.at[0], 1))
        pl.when(has_above)(lambda: greet(s_token.at[0], above))
        pl.when(has_above)(lambda: pl.semaphore_wait(s_token.at[1], 1))
        pl.when(has_below)(lambda: greet(s_token.at[1], below))
    with jax.named_scope("build"):
        build_tiles()
    with jax.named_scope("first"):
        for k in range(EARLY):
            forward(k)
        local_k.wait()
        local_p.wait()
        arrived(wave.at[:, 0], s_loc.at[3])
        arrived(wave.at[pl.ds(0, EARLY), pl.ds(0, 2)], s_wo.at[0])
        acc[...] = jnp.zeros_like(acc)
        each_tile(lambda t: add_product(slice(0, EARLY), 0, columns(t)))
        lax.fori_loop(0, PIECES, turn_own, 0)
    for i in range(PIECES):
        with jax.named_scope(f"piece#i={i}"):
            send_p[i].wait_recv()
            add_product(slice(0, EARLY), 1, slice(i * piece, (i + 1) * piece))
            if i < PIECES - 1:
                turn(1, i)

    def settle(k):
        sent = (proj.at[1], wave.at[:, pl.ds(0, 3)], drecv, parts, drecv, parts)
        for kind, ref in enumerate(sent):
            arrived(ref, s_send.at[kind])

    stages = {
        "forward": forward, "correlate": correlate, "reduce": reduce, "join": join, "mix": mix,
        "share": share_out, "expand": expand, "settle": settle,
    }
    def turn_last(k):
        turn(1, PIECES - 1)

    stages["turn"] = turn_last
    for stage, k, t in schedule():
        with jax.named_scope(f"{stage}#k={k}#t={t}"):
            if stage == "far":
                far(k, t)
            elif stage == "near":
                near(k, t)
            else:
                stages[stage](k)
    with jax.named_scope("others"):
        arrived(nsend, s_send.at[6])
        arrived(nfull, s_send.at[7])
    with jax.named_scope("last"):
        arrived(nfull, s_out.at[0])


def in_hbm(array):
    return pltpu.with_memory_space_constraint(array, pltpu.HBM)


def square(nga, wavefunctions, projectors, kinetic_diag, species_index, coupling):
    bands, waves = wavefunctions.shape
    count = projectors.shape[0]
    atoms = species_index.shape[0]
    half, rows = waves // 2, bands // CHUNKS
    zn = nga // 2
    width, share = half // TILES, 4 * rows // zn
    bf16, f32 = jnp.bfloat16, jnp.float32
    dma = pltpu.SemaphoreType.DMA
    anywhere = pl.BlockSpec(memory_space=pl.ANY)
    return pl.pallas_call(
        functools.partial(kernel, nga),
        out_shape=jax.ShapeDtypeStruct((bands, waves), bf16),
        in_specs=[anywhere] * 5,
        out_specs=pl.BlockSpec(memory_space=pltpu.VMEM),
        scratch_shapes=[
            pltpu.VMEM((2, count, half), bf16),
            pltpu.VMEM((half, 2 * count), bf16),
            pltpu.VMEM((CHUNKS, 4, rows, half), bf16),
            pltpu.VMEM((EARLY, zn, share, 2 * count), f32),
            pltpu.VMEM((CHUNKS, zn, share, 2 * count), bf16),
            pltpu.VMEM((CHUNKS, share, 2 * count), f32),
            pltpu.VMEM((CHUNKS, zn - 1, share, 2 * count), bf16),
            pltpu.VMEM((CHUNKS, share, count), bf16),
            pltpu.VMEM((CHUNKS, share, count), bf16),
            pltpu.VMEM((CHUNKS, share, count), f32),
            pltpu.VMEM((CHUNKS, share, count), f32),
            pltpu.VMEM((CHUNKS, zn, share, 2 * count), bf16),
            pltpu.VMEM((CHUNKS, 2, TILES, rows, width), bf16),
            pltpu.VMEM((CHUNKS, 2, TILES, rows, width), bf16),
            pltpu.VMEM((3, TILES, 2, rows, width), f32),
            pltpu.VMEM((CHUNKS, TILES, rows, width), bf16),
            pltpu.VMEM((1, half), f32),
            pltpu.VMEM((1, atoms), jnp.int32),
            pltpu.VMEM(coupling.shape, f32),
            pltpu.VMEM((count // LANES, LANES, LANES), f32),
            dma((8,)),
            dma((5,)),
            dma((PIECES,)),
            dma((CHUNKS,)),
            dma((CHUNKS - EARLY + 1,)),
            dma((CHUNKS,)),
            dma((CHUNKS,)),
            dma((CHUNKS,)),
            dma((CHUNKS,)),
            dma((CHUNKS,)),
            dma((2 + (CHUNKS - 2) * TILES,)),
            dma((CHUNKS + TILES - 1,)),
            dma((1,)),
            pltpu.SemaphoreType.REGULAR((2,)),
        ],
        compiler_params=pltpu.CompilerParams(
            collective_id=0, has_side_effects=True, vmem_limit_bytes=53_300_000
        ),
    )(
        wavefunctions, projectors, in_hbm(kinetic_diag.reshape(1, waves)),
        in_hbm(species_index.reshape(1, atoms)), in_hbm(coupling),
    )


def solution(mesh):
    in_specs = (P("band", "ga"), P("band", "ga"), P("ga"), P(), P())
    out_specs = P("band", "ga")
    nga = mesh.shape["ga"]
    fits = mesh.shape["band"] == 4 and nga % 8 == 0
    body = functools.partial(square, nga) if fits else local
    return jax.shard_map(body, mesh=mesh, in_specs=in_specs, out_specs=out_specs, check_vma=False)
```
